128 devices in a mesh: col: 64 (over y, x, z), grp: 2 (over core).
Axes of the slice: x: 4, y: 4, z: 4, core: 2. Of those that a mesh axis runs over, the one named last changes fastest.
Arguments:
- diag_blocks: float32 [64, 128, 128], P('col'), as said below
- panel_blocks: float32 [64, 2, 128, 128], P('col', 'grp'), as said below
- targets: int32 [64, 2], replicated, may hold values from 0 to 64, as said below
Outputs:
- factor_diag: float32 [64, 128, 128], P('col')
- factor_panel: float32 [64, 2, 128, 128], P('col', 'grp')
The draws below stay inside these ranges and needn't reach their ends.
Inputs may be any that keep to these rules, and one draw needn't show every extreme that they name: targets[s, 0] is the parent of supernode s and targets[s, 1] = targets[targets[s, 0], 0] its grandparent, 64 where that ancestor lies outside the window; the tree is a binary heap under a random labelling: exactly one root, every supernode has at most two children and at most four grandchildren, and level d holds min(2 ** d, 64 - 2 ** d + 1) supernodes. `diag_blocks`: each block is symmetric positive definite, and every updated diagonal block stays positive definite. `panel_blocks`: every entry lies within 8 / sqrt(128) of zero.
All inputs are finite; a program needn't handle non-finite values.
Results may differ from the reference program's by a relative error of at most 0.00095.
Values may be sent and summed in bfloat16 or wider, within the bound.
A program may use at most 64 MiB of HBM per device.

```python
import jax
import jax.numpy as jnp
from jax import lax

W = 128
NS = 64


def draw_targets(key, part):
    heap_pos = jax.random.permutation(key, NS).astype(jnp.int32)
    labels = jnp.argsort(heap_pos).astype(jnp.int32)
    above = jnp.maximum(heap_pos - 1, 0) // 2
    parent = jnp.where(heap_pos > 0, labels[above], NS).astype(jnp.int32)
    extended = jnp.concatenate([parent, jnp.array([NS], jnp.int32)])
    grand = extended[parent]
    return jnp.stack([parent, grand], 1).astype(jnp.int32)


def draw_diag_blocks(key, part):
    noise_key = jax.random.fold_in(key, 11)
    level_key = jax.random.fold_in(key, 23)
    noise = jax.random.normal(noise_key, (NS, W, W), jnp.float32)
    levels = 8.0 + 8.0 * jax.random.uniform(level_key, (NS, W), jnp.float32)
    symmetric = (noise + jnp.swapaxes(noise, 1, 2)) * (1.0 / 2.0 ** 0.5 / W ** 0.5)
    return (symmetric + levels[:, :, None] * jnp.eye(W, dtype=jnp.float32)[None]).astype(jnp.float32)


def draw_panel_blocks(key, part):
    entry_key = jax.random.fold_in(key, 37)
    spread = 1.8 / W ** 0.5
    values = jnp.clip(jax.random.normal(entry_key, (NS, 2, W, W), jnp.float32), -4.0, 4.0)
    return (values * spread).astype(jnp.float32)


def setup_inputs(seed: int = 0) -> dict:
    arg_keys = jax.random.split(jax.random.key(seed), 4)
    diag_blocks = draw_diag_blocks(jax.random.fold_in(arg_keys[3], 71), 0)
    panel_blocks = draw_panel_blocks(jax.random.fold_in(arg_keys[3], 71), 0)
    targets = draw_targets(jax.random.fold_in(arg_keys[3], 71), 0)
    return {"diag_blocks": diag_blocks, "panel_blocks": panel_blocks, "targets": targets}


def node_depth(parent, nodes):
    extended = jnp.concatenate([parent, jnp.array([nodes], jnp.int32)])
    depth = jnp.zeros((nodes,), jnp.int32)
    current = parent
    for index in range(nodes.bit_length()):
        depth = depth + (current < nodes).astype(jnp.int32)
        current = extended[current]
    return depth

def solve_right(lower, panel):

    def one(factor, block):
        return jax.scipy.linalg.solve_triangular(factor, block.T, lower=True).T
    return jax.vmap(one)(lower, panel)

def rounded(values):
    low = values.astype(jnp.bfloat16)
    low = lax.optimization_barrier(low)
    return low.astype(jnp.float32)

def reference(diag_blocks, panel_blocks, targets):
    parent = targets[:, 0]
    grand = targets[:, 1]
    depth = node_depth(parent, NS)
    acc_diag = diag_blocks
    acc_near = panel_blocks[:, 0]
    far_panel = panel_blocks[:, 1]
    out_diag = jnp.zeros_like(diag_blocks)
    output_panel = jnp.zeros_like(panel_blocks)
    for level in range(NS.bit_length() - 1, -1, -1):
        active_nodes = depth == level
        wide_mask = active_nodes[:, None, None]
        lower = jnp.linalg.cholesky(acc_diag)
        near = solve_right(lower, acc_near)
        far = solve_right(lower, far_panel)
        out_diag = jnp.where(wide_mask, lower, out_diag)
        output_panel = jnp.where(wide_mask[:, None], jnp.stack([near, far], 1), output_panel)
        if level > 0:
            near_low = rounded(jnp.where(wide_mask, near, 0.0))
            far_low = rounded(jnp.where(wide_mask, far, 0.0))
            diag_near = jnp.einsum('cab,cdb->cad', near_low, near_low, precision=lax.Precision.HIGHEST)
            diag_far = jnp.einsum('cab,cdb->cad', far_low, far_low, precision=lax.Precision.HIGHEST)
            cross_far = jnp.einsum('cab,cdb->cad', far_low, near_low, precision=lax.Precision.HIGHEST)
            seg_near = jnp.where(active_nodes, parent, NS)
            seg_far = jnp.where(active_nodes, grand, NS)
            acc_diag = acc_diag - jax.ops.segment_sum(diag_near, seg_near, NS + 1)[:NS]
            acc_diag = acc_diag - jax.ops.segment_sum(diag_far, seg_far, NS + 1)[:NS]
            acc_near = acc_near - jax.ops.segment_sum(cross_far, seg_near, NS + 1)[:NS]
    return (out_diag, output_panel)
```

```python
import jax
import jax.numpy as jnp
from jax import lax
from jax.experimental import pallas as pl
from jax.experimental.pallas import tpu as pltpu
from jax.sharding import PartitionSpec as P

F32, BF16 = jnp.float32, jnp.bfloat16
MESH = pl.DeviceIdType.MESH
W = 128
NODES = 64
LEVELS = 7
BLOCK = 32
PART = 16


def order_kernel(targets, order, count, total, first):
    def clear(i, carry):
        count[i] = 0
        total[i] = 0
        return carry

    lax.fori_loop(0, NODES + 1, clear, 0)

    def enter(s, carry):
        p = targets[s, 0]
        count[p] = count[p] + 1
        total[p] = total[p] + s
        first[p] = s
        return carry

    lax.fori_loop(0, NODES, enter, 0)
    lone = lax.fori_loop(0, NODES, lambda s, x: jnp.where(count[s] == 1, s, x), 0)
    first[lone] = total[lone]
    node = lone
    for _ in range(LEVELS - 2):
        above = targets[node, 0]
        first[above] = node
        node = above
    order[0] = node
    order[NODES - 1] = total[lone]

    def descend(h, carry):
        node = order[h]
        order[2 * h + 1] = first[node]
        order[2 * h + 2] = total[node] - first[node]
        return carry

    lax.fori_loop(0, NODES // 2 - 1, descend, 0)

    def invert(h, carry):
        order[NODES + order[h]] = h
        return carry

    lax.fori_loop(0, NODES, invert, 0)


def heap_order(targets):
    return pl.pallas_call(
        order_kernel,
        out_shape=jax.ShapeDtypeStruct((2 * NODES,), jnp.int32),
        in_specs=[pl.BlockSpec(memory_space=pltpu.SMEM)],
        out_specs=pl.BlockSpec(memory_space=pltpu.SMEM),
        scratch_shapes=[pltpu.SMEM((NODES + 1,), jnp.int32)] * 3,
        name="heap_order",
    )(targets)


def in_three(x):
    high = x.astype(BF16)
    rest = x - high.astype(F32)
    middle = rest.astype(BF16)
    return high, middle, (rest - middle.astype(F32)).astype(BF16)


def wide(x, n):
    return jnp.concatenate([x] * n, axis=1)


def factor(work):
    tall = BLOCK // 8
    row = lax.broadcasted_iota(jnp.int32, (8, W), 0)
    for b in range(W // BLOCK):
        start = b * BLOCK
        x = [work[pl.ds(start + 8 * v, 8), :] for v in range(tall)]
        scale = [None] * tall
        for part in range(0, BLOCK, PART):
            cols = {}
            for k in range(part, part + PART):
                for v in range(k // 8, tall):
                    cols[k, v] = jnp.broadcast_to(x[v][:, start + k : start + k + 1], (8, W))
            for j in range(part, part + PART):
                v0, s = divmod(j, 8)
                r = lax.rsqrt(jnp.broadcast_to(cols[j, v0][s : s + 1, :], (8, W)))
                low = {v: cols[j, v] * r for v in range(v0, tall)}
                below = dict(low)
                below[v0] = jnp.where(row > s, low[v0], 0.0)
                scale[v0] = r if s == 0 else jnp.where(row == s, r, scale[v0])
                pivot = jnp.concatenate(
                    [
                        jnp.broadcast_to(x[v0][s : s + 1, c * W : (c + 1) * W], (8, W)) * r
                        for c in range(3)
                    ],
                    axis=1,
                )
                for k in range(j + 1, part + PART):
                    mult = jnp.broadcast_to(low[k // 8][k % 8 : k % 8 + 1, :], (8, W))
                    for v in range(k // 8, tall):
                        cols[k, v] = cols[k, v] - low[v] * mult
                for v in range(v0, tall):
                    x[v] = x[v] - wide(below[v], 3) * pivot
        for v in range(tall):
            x[v] = x[v] * wide(scale[v], 3)
            work[pl.ds(start + 8 * v, 8), :] = x[v]
        if start + BLOCK < W:
            high, middle, low3 = in_three(jnp.concatenate(x, axis=0))
            right = jnp.concatenate([high, middle, high, low3, middle, high], axis=0)
            left = jnp.concatenate(
                [p[:, :W] for p in (high, high, middle, high, middle, low3)], axis=0
            )
            update = jnp.dot(left.T[start + BLOCK :, :], right, preferred_element_type=F32)
            work[pl.ds(start + BLOCK, W - start - BLOCK), :] -= update


def tree_kernel(
    order,
    diag,
    panel,
    out_diag,
    out_panel,
    by_label,
    by_place,
    back_place,
    back_label,
    held,
    done,
    work,
    kids,
    kids_out,
    spare,
    spare_in,
    spare_out,
    send1,
    recv1,
    send2,
    recv2,
    send_kids,
    recv_kids,
    send_spare,
    recv_spare,
    send3,
    recv3,
    send4,
    recv_diag,
    recv_panel,
):
    col = lax.axis_index("col")
    grp = lax.axis_index("grp")
    y, x, z = col // 16, (col // 4) % 4, col % 4
    passes = (y // 2 + x // 2) == 1
    tile = (y // 2) * 16 + (y % 2) * 8 + (x % 2) * 4 + z
    works = (y // 2 + x // 2) == 0
    role = (1 - grp) + 2 * (z % 2) + 4 * x + 8 * y + 16 * (z // 2)

    def copy(src, dst, send, recv, to):
        return pltpu.make_async_remote_copy(
            src_ref=src, dst_ref=dst, send_sem=send, recv_sem=recv, device_id=to, device_id_type=MESH
        )

    def passer(t, g):
        h = t // 16
        py, px = 2 * h + (t // 8) % 2, 2 * (1 - h) + (t // 4) % 2
        return (py * 16 + px * 4 + t % 4, g)

    def worker(r):
        wz, wx, wy = (r // 2) % 2 + 2 * (r // 16), (r // 4) % 2, (r // 8) % 2
        return (wy * 16 + wx * 4 + wz, 1 - r % 2)

    def rows(n):
        return pl.ds(pl.multiple_of(n * 8, 8), 8)

    def spread(t, carry):
        copy(diag.at[0, rows(t)], by_label.at[col], send1, recv1, passer(t, 1 - grp)).start()
        copy(panel.at[0, 0, rows(t)], by_label.at[col], send1, recv1, passer(16 + t, 1 - grp)).start()
        return carry

    lax.fori_loop(0, 16, spread, 0)

    @pl.when(works)
    def _():
        kids[0] = jnp.zeros((2, 2 * W, W), BF16)
        spare[...] = jnp.zeros((W, W), F32)
        spare_in[0] = jnp.zeros((W, W), F32)

    on_diag = tile < 16
    sends_in = passes & ((tile >= 16) | ((tile < 8) == (grp == 1)))
    held_row = jnp.where(on_diag, tile, 16 + 16 * (1 - grp) + tile - 16)

    @pl.when(passes)
    def _():
        pltpu.make_async_copy(by_label, by_label, recv1).wait()

    @pl.when(sends_in)
    def _():
        def place(h, carry):
            by_place[h] = by_label[order[h]]
            return carry

        lax.fori_loop(0, NODES, place, 0)
        for step in range(LEVELS):
            first = (1 << (6 - step)) - 1
            stride = 1 << max(step - 1, 0)

            def hand_in(i, carry):
                copy(
                    by_place.at[first + i],
                    held.at[step, rows(held_row)],
                    send2,
                    recv2.at[step],
                    worker(i * stride),
                ).start()
                return carry

            lax.fori_loop(0, 1 if step == 0 else first + 1, hand_in, 0)

    def active(step, stride):
        return (role % stride == 0) & ((step > 0) | (role == 0))

    def climb(step, carry):
        stride, first = carry

        @pl.when(active(step, stride))
        def _():
            prev = jnp.maximum(step - 1, 0)
            gives = (role // stride) % 2 == 1
            partner = worker(jnp.maximum(role - stride, 0))
            pltpu.make_async_copy(held.at[step], held.at[step], recv2.at[step]).wait()
            work[:, W : 2 * W] = held[step, W : 2 * W, :].T
            work[:, 2 * W :] = held[step, 2 * W :, :].T

            @pl.when(step > 1)
            def _():
                pltpu.make_async_copy(kids.at[prev, 1], kids.at[prev, 1], recv_kids.at[prev]).wait()
                pltpu.make_async_copy(spare_in.at[prev], spare_in.at[prev], recv_spare.at[prev]).wait()

            near = jnp.concatenate([kids[prev, 0, :W, :], kids[prev, 1, :W, :]], axis=0)
            far = jnp.concatenate([kids[prev, 0, W:, :], kids[prev, 1, W:, :]], axis=0)
            both = jnp.concatenate([near, far], axis=1)
            update = jnp.dot(near.T, both, preferred_element_type=F32)
            ahead = jnp.dot(far.T, far, preferred_element_type=F32)
            work[:, :W] = held[step, :W, :] - (update[:, :W] + (spare[...] + spare_in[prev]))
            work[:, W : 2 * W] -= update[:, W:]

            @pl.when(gives)
            def _():
                spare_out[...] = ahead
                copy(spare_out, spare_in.at[step], send_spare, recv_spare.at[step], partner).start()

            @pl.when(jnp.logical_not(gives))
            def _():
                spare[...] = ahead

            factor(work)

            @pl.when(gives)
            def _():
                kids_out[:W, :] = work[:, W : 2 * W].astype(BF16)
                kids_out[W:, :] = work[:, 2 * W :].astype(BF16)
                copy(kids_out, kids.at[step, 1], send_kids, recv_kids.at[step], partner).start()

            @pl.when(jnp.logical_not(gives))
            def _():
                kids[step, 0, :W, :] = work[:, W : 2 * W].astype(BF16)
                kids[step, 0, W:, :] = work[:, 2 * W :].astype(BF16)

            down = lax.broadcasted_iota(jnp.int32, (W, W), 0)
            across = lax.broadcasted_iota(jnp.int32, (W, W), 1)
            done[step, :W, :] = jnp.where(across >= down, work[:, :W], 0.0).T
            done[step, W : 2 * W, :] = work[:, W : 2 * W].T
            done[step, 2 * W :, :] = work[:, 2 * W :].T
            place = first + role // stride

            def hand_out(t, carry):
                for g in range(2):
                    copy(
                        done.at[step, rows(t)],
                        back_place.at[place],
                        send3.at[step],
                        recv3,
                        passer(t, g),
                    ).start()
                    copy(
                        done.at[step, rows(16 + 16 * g + t)],
                        back_place.at[place],
                        send3.at[step],
                        recv3,
                        passer(16 + t, 1 - g),
                    ).start()
                return carry

            lax.fori_loop(0, 16, hand_out, 0)

        return jnp.where(step == 0, 1, stride * 2), first // 2

    @pl.when(works)
    def _():
        lax.fori_loop(0, LEVELS, climb, (1, NODES - 1))

    @pl.when(passes)
    def _():
        pltpu.make_async_copy(back_place, back_place, recv3).wait()

        def unplace(s, carry):
            back_label[s] = back_place[order[NODES + s]]
            return carry

        lax.fori_loop(0, NODES, unplace, 0)

    @pl.when(passes & on_diag)
    def _():
        def hand_back(s, carry):
            copy(back_label.at[s], out_diag.at[0, rows(tile)], send4, recv_diag, (s, 1 - grp)).start()
            return carry

        lax.fori_loop(0, NODES, hand_back, 0)

    @pl.when(passes & jnp.logical_not(on_diag))
    def _():
        def hand_back(s, carry):
            copy(
                back_label.at[s], out_panel.at[0, 0, rows(tile - 16)], send4, recv_panel, (s, 1 - grp)
            ).start()
            return carry

        lax.fori_loop(0, NODES, hand_back, 0)

    sent = by_label.at[pl.ds(0, 32)]
    pltpu.make_async_copy(sent, sent, send1).wait()

    @pl.when(sends_in)
    def _():
        pltpu.make_async_copy(by_place, by_place, send2).wait()

    @pl.when(works)
    def _():
        def drain(step, stride):
            @pl.when(active(step, stride))
            def _():
                pltpu.make_async_copy(by_label, by_label, send3.at[step]).wait()

            return jnp.where(step == 0, 1, stride * 2)

        lax.fori_loop(0, LEVELS, drain, 1)

        @pl.when(role > 0)
        def _():
            pltpu.make_async_copy(kids_out, kids_out, send_kids).wait()
            pltpu.make_async_copy(spare_out, spare_out, send_spare).wait()

    @pl.when(passes)
    def _():
        pltpu.make_async_copy(back_label, back_label, send4).wait()

    pltpu.make_async_copy(out_diag, out_diag, recv_diag).wait()
    pltpu.make_async_copy(out_panel, out_panel, recv_panel).wait()


def shards(diag_blocks, panel_blocks, targets):
    vmem = pl.BlockSpec(memory_space=pltpu.VMEM)
    dma = pltpu.SemaphoreType.DMA
    tiles = pltpu.VMEM((NODES, 8, W), F32)
    return pl.pallas_call(
        tree_kernel,
        out_shape=(
            jax.ShapeDtypeStruct(diag_blocks.shape, F32),
            jax.ShapeDtypeStruct(panel_blocks.shape, F32),
        ),
        in_specs=[pl.BlockSpec(memory_space=pltpu.SMEM), vmem, vmem],
        out_specs=(vmem, vmem),
        scratch_shapes=[
            tiles,
            tiles,
            tiles,
            tiles,
            pltpu.VMEM((LEVELS, 3 * W, W), F32),
            pltpu.VMEM((LEVELS, 3 * W, W), F32),
            pltpu.VMEM((W, 3 * W), F32),
            pltpu.VMEM((LEVELS, 2, 2 * W, W), BF16),
            pltpu.VMEM((2 * W, W), BF16),
            pltpu.VMEM((W, W), F32),
            pltpu.VMEM((LEVELS, W, W), F32),
            pltpu.VMEM((W, W), F32),
            dma,
            dma,
            dma,
            dma((LEVELS,)),
            dma,
            dma((LEVELS,)),
            dma,
            dma((LEVELS,)),
            dma((LEVELS,)),
            dma,
            dma,
            dma,
            dma,
        ],
        compiler_params=pltpu.CompilerParams(has_side_effects=True),
        name="tree",
    )(heap_order(targets), diag_blocks, panel_blocks)


def solution(mesh):
    placed = (P("col", None, None), P("col", "grp", None, None), P())
    return jax.shard_map(
        shards,
        mesh=mesh,
        in_specs=placed,
        out_specs=(P("col", None, None), P("col", "grp", None, None)),
        check_vma=False,
    )
```

```python
import jax
import jax.numpy as jnp
from jax import lax
from jax.experimental import pallas as pl
from jax.experimental.pallas import tpu as pltpu
from jax.sharding import PartitionSpec as P

F32, BF16 = jnp.float32, jnp.bfloat16
MESH = pl.DeviceIdType.MESH
W = 128
NODES = 64
LEVELS = 7
BLOCK = 32
NEAR_FIRST = tuple(
    tuple(sorted(range(NODES), key=lambda s: (s // 16 + s // 4 % 4 + s % 4, (s * 7 + 16 * turn) % NODES)))
    for turn in range(4)
)
PART = 16


def power_of_two(n, most):
    result = jnp.ones_like(n)
    for k in range(1, most + 1):
        result = result * jnp.where(n >= k, 2.0, 1.0)
    return result


def heap_order(parent):
    def dot(a, b, over):
        return lax.dot_general(
            a.astype(BF16), b.astype(BF16), ((over[:1], over[1:]), ((), ())), preferred_element_type=F32
        )

    down = lax.broadcasted_iota(jnp.int32, (NODES, NODES), 0)
    across = lax.broadcasted_iota(jnp.int32, (NODES, NODES), 1)
    one = (down == parent).astype(F32)
    two = dot(one, one, (1, 0))
    four = dot(two, two, (1, 0))
    alive = jnp.broadcast_to((parent < NODES).astype(F32), (8, NODES))
    len2 = alive + dot(alive, one, (1, 0))
    len4 = len2 + dot(len2, two, (1, 0))
    depth = len4 + dot(len4, four, (1, 0))
    path = (depth == LEVELS - 1).astype(F32)
    for above in (one, two, four):
        path = path + dot(path, above, (1, 1))
    siblings = dot(one, one, (0, 0))
    rank = jnp.sum(jnp.where(down < across, siblings, 0.0), axis=0, keepdims=True)
    beside = dot(path, siblings, (1, 0)) - path * alive
    code = alive * (1.0 - path) * jnp.maximum(beside, rank)
    code = code + (1.0 + alive) * dot(code, one, (1, 0))
    code = code + power_of_two(len2, 2) * dot(code, two, (1, 0))
    code = code + power_of_two(len4, 4) * dot(code, four, (1, 0))
    place = power_of_two(depth, LEVELS - 1) - 1.0 + code
    holds = (down == jnp.broadcast_to(place[:1], (NODES, NODES)).astype(jnp.int32)).astype(F32)
    label = lax.broadcasted_iota(jnp.int32, (8, NODES), 1).astype(F32)
    return dot(label, holds, (1, 1)), place


def in_three(x):
    high = x.astype(BF16)
    rest = x - high.astype(F32)
    middle = rest.astype(BF16)
    return high, middle, (rest - middle.astype(F32)).astype(BF16)


def wide(x, n):
    return jnp.concatenate([x] * n, axis=1)


def factor(work, before_last):
    tall = BLOCK // 8
    row = lax.broadcasted_iota(jnp.int32, (8, W), 0)
    for b in range(W // BLOCK):
        start = b * BLOCK
        if start + BLOCK == W:
            before_last()
        x = [work[pl.ds(start + 8 * v, 8), :] for v in range(tall)]
        scale = [None] * tall
        for part in range(0, BLOCK, PART):
            cols = {}
            for k in range(part, part + PART):
                for v in range(k // 8, tall):
                    cols[k, v] = jnp.broadcast_to(x[v][:, start + k : start + k + 1], (8, W))
            for j in range(part, part + PART):
                v0, s = divmod(j, 8)
                r = lax.rsqrt(jnp.broadcast_to(cols[j, v0][s : s + 1, :], (8, W)))
                low = {v: cols[j, v] * r for v in range(v0, tall)}
                below = dict(low)
                below[v0] = jnp.where(row > s, low[v0], 0.0)
                scale[v0] = r if s == 0 else jnp.where(row == s, r, scale[v0])
                pivot = jnp.concatenate(
                    [
                        jnp.broadcast_to(x[v0][s : s + 1, c * W : (c + 1) * W], (8, W)) * r
                        for c in range(3)
                    ],
                    axis=1,
                )
                for k in range(j + 1, part + PART):
                    mult = jnp.broadcast_to(low[k // 8][k % 8 : k % 8 + 1, :], (8, W))
                    for v in range(k // 8, tall):
                        cols[k, v] = cols[k, v] - low[v] * mult
                for v in range(v0, tall):
                    x[v] = x[v] - wide(below[v], 3) * pivot
        for v in range(tall):
            x[v] = x[v] * wide(scale[v], 3)
            work[pl.ds(start + 8 * v, 8), :] = x[v]
        if start + BLOCK < W:
            high, middle, low3 = in_three(jnp.concatenate(x, axis=0))
            right = jnp.concatenate([high, middle, high, low3, middle, high], axis=0)
            left = jnp.concatenate(
                [p[:, :W] for p in (high, high, middle, high, middle, low3)], axis=0
            )
            update = jnp.dot(left.T[start + BLOCK :, :], right, preferred_element_type=F32)
            work[pl.ds(start + BLOCK, W - start - BLOCK), :] -= update


def tree_kernel(
    targets_in,
    diag_in,
    panel_in,
    out_diag,
    out_panel,
    targets,
    diag,
    panel,
    ranks,
    order,
    load,
    by_label,
    by_place,
    back_place,
    back_label,
    held,
    done,
    work,
    kids,
    kids_out,
    spare,
    spare_in,
    spare_out,
    send1,
    recv1,
    send2,
    recv2,
    send_kids,
    recv_kids,
    send_spare,
    recv_spare,
    send3,
    recv3,
    send4,
    recv_diag,
    recv_panel,
):
    col = lax.axis_index("col")
    grp = lax.axis_index("grp")
    y, x, z = col // 16, (col // 4) % 4, col % 4
    upper_y, upper_x = y // 2, x // 2
    works = (upper_y + upper_x) == 0
    role = (1 - grp) + 2 * (z % 2) + 4 * x + 8 * y + 16 * (z // 2)
    tile = (y % 2) * 8 + (x % 2) * 4 + z
    on_diag = (upper_y + upper_x) == 2
    on_panel = ((upper_y + upper_x) == 1) & (upper_x == grp)
    passes_in = on_panel | (on_diag & ((tile < 8) == (grp == 1)))
    passes_back = on_panel | on_diag
    kind = upper_x + 2 * upper_y
    held_row = tile + 16 * (kind % 3)

    def at(dy, dx, t):
        return (2 * dy + t // 8) * 16 + (2 * dx + (t // 4) % 2) * 4 + t % 4

    def diag_passer(t, g):
        return (at(1, 1, t), g)

    def panel_passer(t, c):
        return (at(c, 1 - c, t), 1 - c)

    def worker(r):
        wz, wx, wy = (r // 2) % 2 + 2 * (r // 16), (r // 4) % 2, (r // 8) % 2
        return (wy * 16 + wx * 4 + wz, 1 - r % 2)

    def within(n):
        return jnp.minimum(jnp.maximum(n, 0), NODES - 1)

    def rows(n):
        return pl.ds(pl.multiple_of(n * 8, 8), 8)

    def copy(src, dst, send, recv, to):
        return pltpu.make_async_remote_copy(
            src_ref=src, dst_ref=dst, send_sem=send, recv_sem=recv, device_id=to, device_id_type=MESH
        )

    def repeat(n, body, group=4):
        def several(i, carry):
            for k in range(group):
                body(i * group + k)
            return carry

        lax.fori_loop(0, n // group, several, 0)

    loads = [
        pltpu.make_async_copy(src, dst, load.at[k])
        for k, (src, dst) in enumerate(((targets_in, targets), (diag_in, diag), (panel_in, panel)))
    ]
    for one in loads:
        one.start()

    barrier = pltpu.get_barrier_semaphore()

    def greet(to):
        pl.semaphore_signal(barrier, inc=1, device_id=to, device_id_type=MESH)

    @pl.when(passes_in)
    def _():
        for s in NEAR_FIRST[0]:
            greet((s, 1 - grp))

    for g in range(2):

        @pl.when(works & (grp == g))
        def _(g=g):
            for t in range(16):
                greet(panel_passer(t, 1 - g))
                if (t < 8) == (g == 1):
                    greet(diag_passer(t, g))

    @pl.when(works)
    def _():
        kids[0] = jnp.zeros((2, W, 2 * W), BF16)
        spare[...] = jnp.zeros((W, W), F32)
        spare_in[0] = jnp.zeros((W, W), F32)

    loads[0].wait()

    @pl.when(passes_back)
    def _():
        with jax.named_scope("order"):
            node, place = heap_order(targets[0:1, :])
            ranks[:, :NODES] = node.astype(jnp.int32)
            ranks[:, NODES:] = place.astype(jnp.int32)
            to_scalar = pltpu.make_async_copy(ranks, order, load.at[3])
            to_scalar.start()
            to_scalar.wait()

    loads[1].wait()
    loads[2].wait()
    with jax.named_scope("barrier"):
        pl.semaphore_wait(barrier, 24 + jnp.where(passes_in, 16, 0))

    def spread_panel(i):
        t = (i + col) % 16
        copy(
            panel.at[0, 0, rows(t)], by_label.at[col], send1, recv1, (at(grp, 1 - grp, t), 1 - grp)
        ).start()

    def spread_diag(i):
        t = 8 * grp + (i + col) % 8
        copy(diag.at[0, rows(t)], by_label.at[col], send1, recv1, diag_passer(t, 1 - grp)).start()

    with jax.named_scope("spread"):
        repeat(8, spread_diag)
        repeat(16, spread_panel)

    @pl.when(passes_in)
    def _():
        with jax.named_scope("wait1"):
            pltpu.make_async_copy(by_label, by_label, recv1).wait()

        def place(h):
            by_place[h] = by_label[within(order[0, h])]

        repeat(NODES, place, 8)

        def hand_in(step, h, r):
            copy(
                by_place.at[h], held.at[step, rows(held_row)], send2.at[step // 2], recv2.at[step], worker(r)
            ).start()

        with jax.named_scope("handin"):
            hand_in(0, NODES - 1, 0)
            for turn in range(4):

                @pl.when((tile + kind) % 4 == turn)
                def _(turn=turn):
                    for i in range(32):
                        r = (i + 8 * turn) % 32
                        hand_in(1, 31 + r, r)

            first = by_place.at[pl.ds(0, 33)]
            pltpu.make_async_copy(first, first, send2.at[0]).wait()
            for step in range(2, LEVELS):
                count = 1 << (6 - step)
                for r in range(count):
                    hand_in(step, count - 1 + r, r << (step - 1))

    def active(step, stride):
        return (role % stride == 0) & ((step > 0) | (role == 0))

    def climb(step, carry):
        stride, first = carry

        @pl.when(active(step, stride))
        def _():
            prev = jnp.maximum(step - 1, 0)
            gives = (role // stride) % 2 == 1
            partner = worker(jnp.maximum(role - stride, 0))
            with jax.named_scope("waitheld"):
                pltpu.make_async_copy(held.at[step], held.at[step], recv2.at[step]).wait()
            work[:, W : 2 * W] = held[step, W : 2 * W, :].T
            work[:, 2 * W :] = held[step, 2 * W :, :].T

            @pl.when(step > 1)
            def _():
                with jax.named_scope("waitkids"):
                    pltpu.make_async_copy(spare_in.at[prev], spare_in.at[prev], recv_spare.at[prev]).wait()
                    for part in range(2):
                        lines = kids.at[prev, 1, pl.ds(96 * part, 96 - 64 * part)]
                        pltpu.make_async_copy(lines, lines, recv_kids.at[prev, part]).wait()

            both = jnp.concatenate([kids[prev, 0], kids[prev, 1]], axis=0)
            update = jnp.dot(both[:, :W].T, both, preferred_element_type=F32)
            work[:, :W] = held[step, :W, :] - (update[:, :W] + (spare[...] + spare_in[prev]))
            work[:, W : 2 * W] -= update[:, W:]
            ahead = jnp.dot(both[:, W:].T, both[:, W:], preferred_element_type=F32)

            @pl.when(gives)
            def _():
                spare_out[...] = ahead
                copy(spare_out, spare_in.at[step], send_spare, recv_spare.at[step], partner).start()

            @pl.when(jnp.logical_not(gives))
            def _():
                spare[...] = ahead

            def give(part):
                lines = pl.ds(96 * part, 96 - 64 * part)

                @pl.when(gives)
                def _():
                    kids_out[lines, :] = work[lines, W:].astype(BF16)
                    copy(
                        kids_out.at[lines],
                        kids.at[step, 1, lines],
                        send_kids.at[part],
                        recv_kids.at[step, part],
                        partner,
                    ).start()

            with jax.named_scope("factor"):
                factor(work, lambda: give(0))
            give(1)

            @pl.when(jnp.logical_not(gives))
            def _():
                kids[step, 0] = work[:, W:].astype(BF16)

            down = lax.broadcasted_iota(jnp.int32, (W, W), 0)
            across = lax.broadcasted_iota(jnp.int32, (W, W), 1)
            done[step, :W, :] = jnp.where(across >= down, work[:, :W], 0.0).T
            done[step, W : 2 * W, :] = work[:, W : 2 * W].T
            done[step, 2 * W :, :] = work[:, 2 * W :].T
            place = first + role // stride

            def hand_out(row, to):
                copy(
                    done.at[step, pl.ds(8 * row, 8)], back_place.at[place], send3.at[step], recv3, to
                ).start()

            with jax.named_scope("handout"):
                for t in range(16):
                    for g in range(2):
                        hand_out(t, diag_passer(t, g))
                        hand_out(16 + 16 * g + t, panel_passer(t, g))

        return jnp.where(step == 0, 1, stride * 2), first // 2

    @pl.when(works)
    def _():
        lax.fori_loop(0, LEVELS, climb, (1, NODES - 1))

    @pl.when(passes_back)
    def _():
        with jax.named_scope("wait3"):
            pltpu.make_async_copy(back_place, back_place, recv3).wait()

        def unplace(s):
            back_label[s] = back_place[within(order[0, NODES + s])]

        repeat(NODES, unplace, 8)

    def hand_back(s, to, recv):
        copy(back_label.at[s], to, send4, recv, (s, 1 - grp)).start()

    for turn in range(4):

        @pl.when(on_diag & (tile % 4 == turn))
        def _(turn=turn):
            for s in NEAR_FIRST[turn]:
                hand_back(s, out_diag.at[0, rows(tile)], recv_diag)

        @pl.when(on_panel & (tile % 4 == turn))
        def _(turn=turn):
            for s in NEAR_FIRST[turn]:
                hand_back(s, out_panel.at[0, 0, rows(tile)], recv_panel)

    sent = by_label.at[pl.ds(0, 24)]
    pltpu.make_async_copy(sent, sent, send1).wait()

    @pl.when(passes_in)
    def _():
        for step in range(1, 4):
            count = (0, 24, 6, 1)[step]
            later = by_place.at[pl.ds(0, count)]
            pltpu.make_async_copy(later, later, send2.at[step]).wait()

    @pl.when(works)
    def _():
        def drain(step, stride):
            @pl.when(active(step, stride))
            def _():
                pltpu.make_async_copy(by_label, by_label, send3.at[step]).wait()

            return jnp.where(step == 0, 1, stride * 2)

        lax.fori_loop(0, LEVELS, drain, 1)

        @pl.when(role > 0)
        def _():
            for part in range(2):
                lines = kids_out.at[pl.ds(96 * part, 96 - 64 * part)]
                pltpu.make_async_copy(lines, lines, send_kids.at[part]).wait()
            pltpu.make_async_copy(spare_out, spare_out, send_spare).wait()

    @pl.when(passes_back)
    def _():
        pltpu.make_async_copy(back_label, back_label, send4).wait()

    with jax.named_scope("waitfinal"):
        pltpu.make_async_copy(out_diag, out_diag, recv_diag).wait()
        pltpu.make_async_copy(out_panel, out_panel, recv_panel).wait()


def shards(diag_blocks, panel_blocks, targets):
    dma = pltpu.SemaphoreType.DMA
    tiles = pltpu.VMEM((NODES, 8, W), F32)
    return pl.pallas_call(
        tree_kernel,
        out_shape=(
            jax.ShapeDtypeStruct(diag_blocks.shape, F32),
            jax.ShapeDtypeStruct(panel_blocks.shape, F32),
        ),
        in_specs=[pl.BlockSpec(memory_space=pl.ANY)] * 3,
        out_specs=(pl.BlockSpec(memory_space=pltpu.VMEM),) * 2,
        scratch_shapes=[
            pltpu.VMEM((2, NODES), jnp.int32),
            pltpu.VMEM(diag_blocks.shape, F32),
            pltpu.VMEM(panel_blocks.shape, F32),
            pltpu.VMEM((8, 2 * NODES), jnp.int32),
            pltpu.SMEM((8, 2 * NODES), jnp.int32),
            dma((4,)),
            tiles,
            tiles,
            tiles,
            tiles,
            pltpu.VMEM((LEVELS, 3 * W, W), F32),
            pltpu.VMEM((LEVELS, 3 * W, W), F32),
            pltpu.VMEM((W, 3 * W), F32),
            pltpu.VMEM((LEVELS, 2, W, 2 * W), BF16),
            pltpu.VMEM((W, 2 * W), BF16),
            pltpu.VMEM((W, W), F32),
            pltpu.VMEM((LEVELS, W, W), F32),
            pltpu.VMEM((W, W), F32),
            dma,
            dma,
            dma((4,)),
            dma((LEVELS,)),
            dma((2,)),
            dma((LEVELS, 2)),
            dma,
            dma((LEVELS,)),
            dma((LEVELS,)),
            dma,
            dma,
            dma,
            dma,
        ],
        compiler_params=pltpu.CompilerParams(collective_id=0, has_side_effects=True),
        name="tree",
    )(targets.T, diag_blocks, panel_blocks)


def solution(mesh):
    placed = (P("col", None, None), P("col", "grp", None, None), P())
    return jax.shard_map(
        shards,
        mesh=mesh,
        in_specs=placed,
        out_specs=(P("col", None, None), P("col", "grp", None, None)),
        check_vma=False,
    )
```

```python
import jax
import jax.numpy as jnp
from jax import lax
from jax.experimental import pallas as pl
from jax.experimental.pallas import tpu as pltpu
from jax.sharding import PartitionSpec as P

F32, BF16 = jnp.float32, jnp.bfloat16
MESH = pl.DeviceIdType.MESH
W = 128
NODES = 64
LEVELS = 7
BLOCK = 32
NEAR_FIRST = tuple(
    tuple(sorted(range(NODES), key=lambda s: (s // 16 + s // 4 % 4 + s % 4, (s * 7 + 16 * turn) % NODES)))
    for turn in range(4)
)
PART = 16


def power_of_two(n, most):
    result = jnp.ones_like(n)
    for k in range(1, most + 1):
        result = result * jnp.where(n >= k, 2.0, 1.0)
    return result


def heap_order(parent):
    def dot(a, b, over):
        return lax.dot_general(
            a.astype(BF16), b.astype(BF16), ((over[:1], over[1:]), ((), ())), preferred_element_type=F32
        )

    down = lax.broadcasted_iota(jnp.int32, (NODES, NODES), 0)
    across = lax.broadcasted_iota(jnp.int32, (NODES, NODES), 1)
    one = (down == parent).astype(F32)
    two = dot(one, one, (1, 0))
    four = dot(two, two, (1, 0))
    alive = jnp.broadcast_to((parent < NODES).astype(F32), (8, NODES))
    len2 = alive + dot(alive, one, (1, 0))
    len4 = len2 + dot(len2, two, (1, 0))
    depth = len4 + dot(len4, four, (1, 0))
    path = (depth == LEVELS - 1).astype(F32)
    for above in (one, two, four):
        path = path + dot(path, above, (1, 1))
    siblings = dot(one, one, (0, 0))
    rank = jnp.sum(jnp.where(down < across, siblings, 0.0), axis=0, keepdims=True)
    beside = dot(path, siblings, (1, 0)) - path * alive
    code = alive * (1.0 - path) * jnp.maximum(beside, rank)
    code = code + (1.0 + alive) * dot(code, one, (1, 0))
    code = code + power_of_two(len2, 2) * dot(code, two, (1, 0))
    code = code + power_of_two(len4, 4) * dot(code, four, (1, 0))
    place = power_of_two(depth, LEVELS - 1) - 1.0 + code
    holds = (down == jnp.broadcast_to(place[:1], (NODES, NODES)).astype(jnp.int32)).astype(F32)
    label = lax.broadcasted_iota(jnp.int32, (8, NODES), 1).astype(F32)
    return dot(label, holds, (1, 1)), place


def in_three(x):
    high = x.astype(BF16)
    rest = x - high.astype(F32)
    middle = rest.astype(BF16)
    return high, middle, (rest - middle.astype(F32)).astype(BF16)


def wide(x, n):
    return jnp.concatenate([x] * n, axis=1)


def factor(work, after_block):
    tall = BLOCK // 8
    row = lax.broadcasted_iota(jnp.int32, (8, W), 0)

    def line(x, s):
        return jnp.broadcast_to(x[s : s + 1, :], (8, W))

    for b in range(W // BLOCK):
        start = b * BLOCK
        if b > 0:
            after_block(b - 1)
        x = [work[pl.ds(start + 8 * v, 8), :] for v in range(tall)]
        pivots = [None] * tall
        for part in range(0, BLOCK, PART):
            cols = {}
            for k in range(part, part + PART):
                for v in range(k // 8, tall):
                    cols[k, v] = jnp.broadcast_to(x[v][:, start + k : start + k + 1], (8, W))
            d = line(cols[part, part // 8], part % 8)
            for j in range(part, part + PART):
                v0, s = divmod(j, 8)
                r = lax.rsqrt(d)
                r2 = r * r
                pivots[v0] = d if s == 0 else jnp.where(row == s, d, pivots[v0])
                mult = {v: cols[j, v] * r2 for v in range(v0, tall)}
                below = dict(mult)
                below[v0] = jnp.where(row > s, mult[v0], 0.0)
                across = {k: line(cols[j, k // 8], k % 8) for k in range(j + 1, part + PART)}
                if j + 1 < part + PART:
                    near = across[j + 1]
                    d = line(cols[j + 1, (j + 1) // 8], (j + 1) % 8) - (near * near) * r2
                for k in range(j + 1, part + PART):
                    for v in range(k // 8, tall):
                        cols[k, v] = cols[k, v] - mult[v] * across[k]
                pivot = jnp.concatenate([line(x[v0][:, c * W : (c + 1) * W], s) for c in range(3)], axis=1)
                for v in range(v0, tall):
                    x[v] = x[v] - wide(below[v], 3) * pivot
        for v in range(tall):
            x[v] = x[v] * wide(lax.rsqrt(pivots[v]), 3)
            work[pl.ds(start + 8 * v, 8), :] = x[v]
        if start + BLOCK < W:
            high, middle, low3 = in_three(jnp.concatenate(x, axis=0))
            right = jnp.concatenate([high, middle, high, low3, middle, high], axis=0)
            left = jnp.concatenate(
                [p[:, :W] for p in (high, high, middle, high, middle, low3)], axis=0
            )
            update = jnp.dot(left.T[start + BLOCK :, :], right, preferred_element_type=F32)
            work[pl.ds(start + BLOCK, W - start - BLOCK), :] -= update


def tree_kernel(
    targets_in,
    diag_in,
    panel_in,
    out_diag,
    out_panel,
    targets,
    diag,
    panel,
    turned,
    got_diag,
    got_panel,
    ranks,
    order,
    by_label,
    by_place,
    back_place,
    back_label,
    work,
    kids,
    spare,
    spare_in,
    load,
    send1,
    recv1,
    send2,
    recv2,
    send_kids,
    recv_kids,
    send_spare,
    recv_spare,
    send3,
    recv3,
    send4,
    recv_diag,
    recv_panel,
):
    col = lax.axis_index("col")
    grp = lax.axis_index("grp")
    y, x, z = col // 16, (col // 4) % 4, col % 4
    upper_z, upper_x = z // 2, x // 2
    works = (upper_z + upper_x) == 2
    role = (
        (1 - grp) + 2 * (z % 2) + 4 * (x % 2) + 8 * (y // 2) + 16 * jnp.where(y % 3 == 0, 1, 0)
    )
    tile = (z % 2) + 2 * (x % 2) + 4 * y
    on_diag = (upper_z + upper_x) == 0
    on_panel = ((upper_z + upper_x) == 1) & (upper_x == grp)
    passes_in = on_panel | (on_diag & ((tile < 8) == (grp == 1)))
    passes_back = on_panel | on_diag
    kind = upper_x + 2 * upper_z
    lanes = pl.ds(pl.multiple_of(W * (kind % 3), W), W)

    def at(dz, dx, t):
        return (t // 4) * 16 + (2 * dx + (t // 2) % 2) * 4 + 2 * dz + t % 2

    def diag_passer(t, g):
        return (at(0, 0, t), g)

    def panel_passer(t, c):
        return (at(c, 1 - c, t), 1 - c)

    def worker(r):
        b3, b4 = (r // 8) % 2, r // 16
        wy = (1 - b4) * (1 + b3) + 3 * b4 * b3
        return (wy * 16 + (2 + (r // 4) % 2) * 4 + 2 + (r // 2) % 2, 1 - r % 2)

    def within(n):
        return jnp.minimum(jnp.maximum(n, 0), NODES - 1)

    def rows(n):
        return pl.ds(pl.multiple_of(n * 8, 8), 8)

    def copy(src, dst, send, recv, to):
        return pltpu.make_async_remote_copy(
            src_ref=src, dst_ref=dst, send_sem=send, recv_sem=recv, device_id=to, device_id_type=MESH
        )

    def repeat(n, body, group=4):
        def several(i, carry):
            for k in range(group):
                body(i * group + k)
            return carry

        lax.fori_loop(0, n // group, several, 0)

    loads = [
        pltpu.make_async_copy(src, dst, load.at[k])
        for k, (src, dst) in enumerate(((targets_in, targets), (diag_in, diag), (panel_in, panel)))
    ]
    for one in loads:
        one.start()

    barrier = pltpu.get_barrier_semaphore()

    def greet(to):
        pl.semaphore_signal(barrier, inc=1, device_id=to, device_id_type=MESH)

    @pl.when(passes_in)
    def _():
        for s in NEAR_FIRST[0]:
            greet((s, 1 - grp))

    greet((col, 1 - grp))

    @pl.when(works)
    def _():
        kids[0] = jnp.zeros((2, W, 2 * W), BF16)
        spare[0] = jnp.zeros((W, W), F32)
        spare_in[0] = jnp.zeros((W, W), F32)

    loads[0].wait()

    @pl.when(passes_back)
    def _():
        with jax.named_scope("order"):
            node, place = heap_order(targets[0:1, :])
            ranks[:, :NODES] = node.astype(jnp.int32)
            ranks[:, NODES:] = place.astype(jnp.int32)
            to_scalar = pltpu.make_async_copy(ranks, order, load.at[3])
            to_scalar.start()
            to_scalar.wait()

    loads[1].wait()
    loads[2].wait()
    turned[...] = panel[0, 0].T
    with jax.named_scope("barrier"):
        pl.semaphore_wait(barrier, 24 + 1)

    def spread_panel(i):
        t = (i + col) % 16
        copy(
            turned.at[rows(t)], by_label.at[col], send1, recv1, (at(grp, 1 - grp, t), 1 - grp)
        ).start()

    def spread_diag(i):
        t = 8 * grp + (i + col) % 8
        copy(diag.at[0, rows(t)], by_label.at[col], send1, recv1, diag_passer(t, 1 - grp)).start()

    with jax.named_scope("spread"):
        repeat(8, spread_diag)
        repeat(16, spread_panel)

    def came_back(step):
        tiles = back_place.at[pl.ds(0, 1 if step == 0 else 1 << (6 - step))]
        pltpu.make_async_copy(tiles, tiles, recv3.at[step]).wait()

    @pl.when(passes_in)
    def _():
        with jax.named_scope("wait1"):
            pltpu.make_async_copy(by_label, by_label, recv1).wait()

        def place(h):
            by_place[h] = by_label[within(order[0, h])]

        for h in range(NODES):
            place(h)

        def hand_in(step, h, r):
            copy(
                by_place.at[h], work.at[step, rows(tile), lanes], send2.at[max(step - 1, 0)], recv2.at[step], worker(r)
            ).start()

        with jax.named_scope("handin"):
            hand_in(0, NODES - 1, 0)
            for turn in range(4):

                @pl.when((tile + kind) % 4 == turn)
                def _(turn=turn):
                    for i in range(32):
                        r = (i + 8 * turn) % 32
                        hand_in(1, 31 + r, r)

            first = by_place.at[pl.ds(0, 33)]
            pltpu.make_async_copy(first, first, send2.at[0]).wait()
            for step in range(2, LEVELS):
                count = 1 << (6 - step)
                if step in (3, 4):
                    left = by_place.at[pl.ds(0, 2 * count)]
                    pltpu.make_async_copy(left, left, send2.at[step - 2]).wait()
                for r in range(count):
                    hand_in(step, count - 1 + r, r << (step - 1))

    def active(step, stride):
        return (role % stride == 0) & ((step > 0) | (role == 0))

    def climb(step, carry):
        stride, first = carry

        @pl.when(active(step, stride))
        def _():
            prev = jnp.maximum(step - 1, 0)
            gives = (role // stride) % 2 == 1
            partner = worker(jnp.maximum(role - stride, 0))
            mine = work.at[step]
            with jax.named_scope("waitheld"):
                pltpu.make_async_copy(mine, mine, recv2.at[step]).wait()

            @pl.when(step > 1)
            def _():
                with jax.named_scope("waitkids"):
                    pltpu.make_async_copy(spare_in.at[prev], spare_in.at[prev], recv_spare.at[prev]).wait()
                    for block in range(W // BLOCK):
                        lines = kids.at[prev, 1, pl.ds(BLOCK * block, BLOCK)]
                        pltpu.make_async_copy(lines, lines, recv_kids.at[prev, block]).wait()

            both = jnp.concatenate([kids[prev, 0], kids[prev, 1]], axis=0)
            update = jnp.dot(both[:, :W].T, both, preferred_element_type=F32)
            work[step, :, :W] -= update[:, :W] + (spare[prev] + spare_in[prev])
            work[step, :, W : 2 * W] -= update[:, W:]
            spare[step] = jnp.dot(both[:, W:].T, both[:, W:], preferred_element_type=F32)

            def give(block):
                lines = pl.ds(BLOCK * block, BLOCK)
                kids[step, 0, lines, :] = mine[lines, W:].astype(BF16)

                @pl.when(gives)
                def _():
                    if block == 0:
                        copy(
                            spare.at[step], spare_in.at[step], send_spare, recv_spare.at[step], partner
                        ).start()
                    copy(
                        kids.at[step, 0, lines],
                        kids.at[step, 1, lines],
                        send_kids.at[block],
                        recv_kids.at[step, block],
                        partner,
                    ).start()

            with jax.named_scope("factor"):
                factor(mine, give)
            give(W // BLOCK - 1)
            place = first + role // stride

            def hand_out(t, c, to):
                copy(
                    work.at[step, pl.ds(8 * t, 8), pl.ds(W * c, W)],
                    back_place.at[place],
                    send3.at[step],
                    recv3.at[step],
                    to,
                ).start()

            with jax.named_scope("handout"):
                for t in range(16):
                    for g in range(2):
                        hand_out(t, 0, diag_passer(t, g))
                        hand_out(t, 1 + g, panel_passer(t, g))

        return jnp.where(step == 0, 1, stride * 2), first // 2

    @pl.when(works)
    def _():
        lax.fori_loop(0, LEVELS, climb, (1, NODES - 1))

    @pl.when(passes_back)
    def _():
        with jax.named_scope("wait3"):
            for step in range(LEVELS):
                came_back(step)

        def unplace(s):
            back_label[s] = back_place[within(order[0, NODES + s])]

        for s in range(NODES):
            unplace(s)

    def hand_back(s, to, recv):
        copy(back_label.at[s], to, send4, recv, (s, 1 - grp)).start()

    for turn in range(4):

        @pl.when(on_diag & (tile % 4 == turn))
        def _(turn=turn):
            for s in NEAR_FIRST[turn]:
                hand_back(s, got_diag.at[rows(tile)], recv_diag)

        @pl.when(on_panel & (tile % 4 == turn))
        def _(turn=turn):
            for s in NEAR_FIRST[turn]:
                hand_back(s, got_panel.at[rows(tile)], recv_panel)

    with jax.named_scope("waitfinal"):
        pltpu.make_async_copy(got_diag, got_diag, recv_diag).wait()
        pltpu.make_async_copy(got_panel, got_panel, recv_panel).wait()
    down = lax.broadcasted_iota(jnp.int32, (W, W), 0)
    across = lax.broadcasted_iota(jnp.int32, (W, W), 1)
    out_diag[0] = jnp.where(across >= down, got_diag[...], 0.0).T
    out_panel[0, 0] = got_panel[...].T

    sent = by_label.at[pl.ds(0, 24)]
    pltpu.make_async_copy(sent, sent, send1).wait()

    @pl.when(passes_in)
    def _():
        for step in range(4, LEVELS):
            later = by_place.at[pl.ds(0, 1 << (6 - step))]
            pltpu.make_async_copy(later, later, send2.at[step - 1]).wait()

    @pl.when(works)
    def _():
        def drain(step, stride):
            @pl.when(active(step, stride))
            def _():
                pltpu.make_async_copy(by_label, by_label, send3.at[step]).wait()

            return jnp.where(step == 0, 1, stride * 2)

        lax.fori_loop(0, LEVELS, drain, 1)

        @pl.when(role > 0)
        def _():
            for block in range(W // BLOCK):
                lines = kids.at[0, 0, pl.ds(BLOCK * block, BLOCK)]
                pltpu.make_async_copy(lines, lines, send_kids.at[block]).wait()
            pltpu.make_async_copy(spare.at[0], spare.at[0], send_spare).wait()

    @pl.when(passes_back)
    def _():
        pltpu.make_async_copy(back_label, back_label, send4).wait()


def shards(diag_blocks, panel_blocks, targets):
    dma = pltpu.SemaphoreType.DMA
    tiles = pltpu.VMEM((NODES, 8, W), F32)
    return pl.pallas_call(
        tree_kernel,
        out_shape=(
            pltpu.VMEM(diag_blocks.shape, F32),
            pltpu.VMEM(panel_blocks.shape, F32),
        ),
        in_specs=[pl.BlockSpec(memory_space=pl.ANY)] * 3,
        out_specs=(pl.BlockSpec(memory_space=pltpu.VMEM),) * 2,
        scratch_shapes=[
            pltpu.VMEM((2, NODES), jnp.int32),
            pltpu.VMEM(diag_blocks.shape, F32),
            pltpu.VMEM(panel_blocks.shape, F32),
            pltpu.VMEM((W, W), F32),
            pltpu.VMEM((W, W), F32),
            pltpu.VMEM((W, W), F32),
            pltpu.VMEM((8, 2 * NODES), jnp.int32),
            pltpu.SMEM((8, 2 * NODES), jnp.int32),
            tiles,
            tiles,
            tiles,
            tiles,
            pltpu.VMEM((LEVELS, W, 3 * W), F32),
            pltpu.VMEM((LEVELS, 2, W, 2 * W), BF16),
            pltpu.VMEM((LEVELS, W, W), F32),
            pltpu.VMEM((LEVELS, W, W), F32),
            dma((4,)),
            dma,
            dma,
            dma((LEVELS - 1,)),
            dma((LEVELS,)),
            dma((W // BLOCK,)),
            dma((LEVELS, W // BLOCK)),
            dma,
            dma((LEVELS,)),
            dma((LEVELS,)),
            dma((LEVELS,)),
            dma,
            dma,
            dma,
        ],
        compiler_params=pltpu.CompilerParams(collective_id=0, has_side_effects=True),
        name="tree",
    )(targets.T, diag_blocks, panel_blocks)


def solution(mesh):
    placed = (P("col", None, None), P("col", "grp", None, None), P())
    return jax.shard_map(
        shards,
        mesh=mesh,
        in_specs=placed,
        out_specs=(P("col", None, None), P("col", "grp", None, None)),
        check_vma=False,
    )
```

```python
import jax
import jax.numpy as jnp
from jax import lax
from jax.experimental import pallas as pl
from jax.experimental.pallas import tpu as pltpu
from jax.sharding import PartitionSpec as P

F32, BF16 = jnp.float32, jnp.bfloat16
MESH = pl.DeviceIdType.MESH
W = 128
NODES = 64
LEVELS = 7
BLOCK = 32
NEAR_FIRST = tuple(
    tuple(sorted(range(NODES), key=lambda s: (s // 16 + s // 4 % 4 + s % 4, (s * 7 + 16 * turn) % NODES)))
    for turn in range(4)
)
PART = 16


def power_of_two(n, most):
    result = jnp.ones_like(n)
    for k in range(1, most + 1):
        result = result * jnp.where(n >= k, 2.0, 1.0)
    return result


def heap_order(parent):
    def dot(a, b, over):
        return lax.dot_general(
            a.astype(BF16), b.astype(BF16), ((over[:1], over[1:]), ((), ())), preferred_element_type=F32
        )

    down = lax.broadcasted_iota(jnp.int32, (NODES, NODES), 0)
    across = lax.broadcasted_iota(jnp.int32, (NODES, NODES), 1)
    one = (down == parent).astype(F32)
    two = dot(one, one, (1, 0))
    four = dot(two, two, (1, 0))
    alive = jnp.broadcast_to((parent < NODES).astype(F32), (8, NODES))
    len2 = alive + dot(alive, one, (1, 0))
    len4 = len2 + dot(len2, two, (1, 0))
    depth = len4 + dot(len4, four, (1, 0))
    path = (depth == LEVELS - 1).astype(F32)
    for above in (one, two, four):
        path = path + dot(path, above, (1, 1))
    siblings = dot(one, one, (0, 0))
    rank = jnp.sum(jnp.where(down < across, siblings, 0.0), axis=0, keepdims=True)
    beside = dot(path, siblings, (1, 0)) - path * alive
    code = alive * (1.0 - path) * jnp.maximum(beside, rank)
    code = code + (1.0 + alive) * dot(code, one, (1, 0))
    code = code + power_of_two(len2, 2) * dot(code, two, (1, 0))
    code = code + power_of_two(len4, 4) * dot(code, four, (1, 0))
    place = power_of_two(depth, LEVELS - 1) - 1.0 + code
    holds = (down == jnp.broadcast_to(place[:1], (NODES, NODES)).astype(jnp.int32)).astype(F32)
    label = lax.broadcasted_iota(jnp.int32, (8, NODES), 1).astype(F32)
    return dot(label, holds, (1, 1)), place


def in_three(x):
    high = x.astype(BF16)
    rest = x - high.astype(F32)
    middle = rest.astype(BF16)
    return high, middle, (rest - middle.astype(F32)).astype(BF16)


def wide(x, n):
    return jnp.concatenate([x] * n, axis=1)


def factor(work, after_block):
    tall = BLOCK // 8
    row = lax.broadcasted_iota(jnp.int32, (8, W), 0)

    def line(x, s):
        return jnp.broadcast_to(x[s : s + 1, :], (8, W))

    for b in range(W // BLOCK):
        start = b * BLOCK
        if b > 0:
            after_block(b - 1)
        x = [work[pl.ds(start + 8 * v, 8), :] for v in range(tall)]
        pivots = [None] * tall
        for part in range(0, BLOCK, PART):
            cols = {}
            for k in range(part, part + PART):
                lane = jnp.full((8, W), start + k, jnp.int32)
                for v in range(k // 8, tall):
                    cols[k, v] = jnp.take_along_axis(x[v][:, :W], lane, axis=1)
            d = line(cols[part, part // 8], part % 8)
            for j in range(part, part + PART):
                v0, s = divmod(j, 8)
                r = lax.rsqrt(d)
                r2 = r * r
                pivots[v0] = d if s == 0 else jnp.where(row == s, d, pivots[v0])
                mult = {v: cols[j, v] * r2 for v in range(v0, tall)}
                below = dict(mult)
                below[v0] = jnp.where(row > s, mult[v0], 0.0)
                across = {k: line(cols[j, k // 8], k % 8) for k in range(j + 1, part + PART)}
                if j + 1 < part + PART:
                    near = across[j + 1]
                    d = line(cols[j + 1, (j + 1) // 8], (j + 1) % 8) - (near * near) * r2
                for k in range(j + 1, part + PART):
                    for v in range(k // 8, tall):
                        cols[k, v] = cols[k, v] - mult[v] * across[k]
                pivot = jnp.concatenate([line(x[v0][:, c * W : (c + 1) * W], s) for c in range(3)], axis=1)
                for v in range(v0, tall):
                    x[v] = x[v] - wide(below[v], 3) * pivot
        for v in range(tall):
            x[v] = x[v] * wide(lax.rsqrt(pivots[v]), 3)
            work[pl.ds(start + 8 * v, 8), :] = x[v]
        if start + BLOCK < W:
            high, middle, low3 = in_three(jnp.concatenate(x, axis=0))
            right = jnp.concatenate([high, middle, high, low3, middle, high], axis=0)
            left = jnp.concatenate(
                [p[:, :W] for p in (high, high, middle, high, middle, low3)], axis=0
            )
            update = jnp.dot(left.T[start + BLOCK :, :], right, preferred_element_type=F32)
            work[pl.ds(start + BLOCK, W - start - BLOCK), :] -= update


def tree_kernel(
    targets_in,
    diag_in,
    panel_in,
    out_diag,
    out_panel,
    targets,
    diag,
    panel,
    turned,
    got_diag,
    got_panel,
    ranks,
    order,
    by_label,
    by_place,
    back_place,
    back_label,
    work,
    kids,
    spare,
    spare_in,
    load,
    send1,
    recv1,
    send2,
    recv2,
    send_kids,
    recv_kids,
    send_spare,
    recv_spare,
    send3,
    recv3,
    send4,
    recv_diag,
    recv_panel,
):
    col = lax.axis_index("col")
    grp = lax.axis_index("grp")
    y, x, z = col // 16, (col // 4) % 4, col % 4
    upper_z, upper_x = z // 2, x // 2
    works = (upper_z + upper_x) == 2
    role = (
        (1 - grp) + 2 * (z % 2) + 4 * (x % 2) + 8 * (y // 2) + 16 * jnp.where(y % 3 == 0, 1, 0)
    )
    tile = (z % 2) + 2 * (x % 2) + 4 * ((y + 2) % 4)
    on_diag = (upper_z + upper_x) == 0
    on_panel = ((upper_z + upper_x) == 1) & (upper_x == grp)
    passes_in = on_panel | (on_diag & ((tile < 8) == (grp == 1)))
    passes_back = on_panel | on_diag
    kind = jnp.where(on_panel, 2 - grp, 0)
    lanes = pl.ds(pl.multiple_of(W * kind, W), W)

    def at(dz, dx, t):
        return ((t // 4 + 2) % 4) * 16 + (2 * dx + (t // 2) % 2) * 4 + 2 * dz + t % 2

    def diag_passer(t, g):
        return (at(0, 0, t), g)

    def panel_passer(t, c):
        return (at(c, 1 - c, t), 1 - c)

    def worker(r):
        b3, b4 = (r // 8) % 2, r // 16
        wy = (1 - b4) * (1 + b3) + 3 * b4 * b3
        return (wy * 16 + (2 + (r // 4) % 2) * 4 + 2 + (r // 2) % 2, 1 - r % 2)

    def within(n):
        return jnp.minimum(jnp.maximum(n, 0), NODES - 1)

    def rows(n):
        return pl.ds(pl.multiple_of(n * 8, 8), 8)

    def copy(src, dst, send, recv, to):
        return pltpu.make_async_remote_copy(
            src_ref=src, dst_ref=dst, send_sem=send, recv_sem=recv, device_id=to, device_id_type=MESH
        )

    def repeat(n, body, group=4):
        def several(i, carry):
            for k in range(group):
                body(i * group + k)
            return carry

        lax.fori_loop(0, n // group, several, 0)

    loads = [
        pltpu.make_async_copy(src, dst, load.at[k])
        for k, (src, dst) in enumerate(((targets_in, targets), (diag_in, diag), (panel_in, panel)))
    ]
    for one in loads:
        one.start()

    barrier = pltpu.get_barrier_semaphore()

    def greet(to):
        pl.semaphore_signal(barrier, inc=1, device_id=to, device_id_type=MESH)

    @pl.when(passes_in)
    def _():
        for s in NEAR_FIRST[0]:
            greet((s, 1 - grp))

    greet((col, 1 - grp))

    @pl.when(works)
    def _():
        kids[0] = jnp.zeros((2, W, 2 * W), BF16)
        spare[0] = jnp.zeros((W, W), F32)
        spare_in[0] = jnp.zeros((W, W), F32)

    loads[1].wait()
    loads[2].wait()
    turned[...] = panel[0, 0].T
    with jax.named_scope("barrier"):
        pl.semaphore_wait(barrier, 24 + 1)

    def spread_panel(i):
        t = (i + col) % 16
        copy(turned.at[rows(t)], by_label.at[col], send1, recv1, (at(grp, 1 - grp, t), 1 - grp)).start()

    def spread_diag(i):
        t = 8 * grp + (i + col) % 8
        copy(diag.at[0, rows(t)], by_label.at[col], send1, recv1, diag_passer(t, 1 - grp)).start()

    with jax.named_scope("spread"):
        repeat(8, spread_diag)
        repeat(16, spread_panel)

    loads[0].wait()

    @pl.when(passes_back)
    def _():
        with jax.named_scope("order"):
            node, place = heap_order(targets[0:1, :])
            ranks[:, :NODES] = node.astype(jnp.int32)
            ranks[:, NODES:] = place.astype(jnp.int32)
            to_scalar = pltpu.make_async_copy(ranks, order, load.at[3])
            to_scalar.start()
            to_scalar.wait()

    def came_back(step):
        tiles = back_place.at[pl.ds(0, 1 if step == 0 else 1 << (6 - step))]
        pltpu.make_async_copy(tiles, tiles, recv3.at[step]).wait()

    @pl.when(passes_in)
    def _():
        with jax.named_scope("wait1"):
            pltpu.make_async_copy(by_label, by_label, recv1).wait()

        def place(h):
            by_place[h] = by_label[within(order[0, h])]

        for h in range(NODES):
            place(h)

        def hand_in(step, h, r):
            copy(
                by_place.at[h], work.at[step, rows(tile), lanes], send2.at[max(step - 1, 0)], recv2.at[step], worker(r)
            ).start()

        with jax.named_scope("handin"):
            hand_in(0, NODES - 1, 0)
            for turn in range(4):

                @pl.when((tile + kind) % 4 == turn)
                def _(turn=turn):
                    for i in range(32):
                        r = (i + 8 * turn) % 32
                        hand_in(1, 31 + r, r)

            first = by_place.at[pl.ds(0, 33)]
            pltpu.make_async_copy(first, first, send2.at[0]).wait()
            for step in range(2, LEVELS):
                count = 1 << (6 - step)
                if step in (3, 4):
                    left = by_place.at[pl.ds(0, 2 * count)]
                    pltpu.make_async_copy(left, left, send2.at[step - 2]).wait()
                for r in range(count):
                    hand_in(step, count - 1 + r, r << (step - 1))

    def active(step, stride):
        return (role % stride == 0) & ((step > 0) | (role == 0))

    def climb(step, carry):
        stride, first = carry

        @pl.when(active(step, stride))
        def _():
            prev = jnp.maximum(step - 1, 0)
            gives = (role // stride) % 2 == 1
            partner = worker(jnp.maximum(role - stride, 0))
            place = first + role // stride
            mine = work.at[step]
            with jax.named_scope("waitheld"):
                pltpu.make_async_copy(mine, mine, recv2.at[step]).wait()

            @pl.when(step > 1)
            def _():
                with jax.named_scope("waitkids"):
                    pltpu.make_async_copy(spare_in.at[prev], spare_in.at[prev], recv_spare.at[prev]).wait()
                    for block in range(W // BLOCK):
                        lines = kids.at[prev, 1, pl.ds(BLOCK * block, BLOCK)]
                        pltpu.make_async_copy(lines, lines, recv_kids.at[prev, block]).wait()

            both = jnp.concatenate([kids[prev, 0], kids[prev, 1]], axis=0)
            update = jnp.dot(both[:, :W].T, both, preferred_element_type=F32)
            work[step, :, :W] -= update[:, :W] + (spare[prev] + spare_in[prev])
            work[step, :, W : 2 * W] -= update[:, W:]
            spare[step] = jnp.dot(both[:, W:].T, both[:, W:], preferred_element_type=F32)

            def hand_out(t, c, to):
                copy(
                    work.at[step, pl.ds(8 * t, 8), pl.ds(W * c, W)],
                    back_place.at[place],
                    send3.at[step],
                    recv3.at[step],
                    to,
                ).start()

            def give(block):
                lines = pl.ds(BLOCK * block, BLOCK)
                kids[step, 0, lines, :] = mine[lines, W:].astype(BF16)

                @pl.when(gives)
                def _():
                    if block == 0:
                        copy(
                            spare.at[step], spare_in.at[step], send_spare, recv_spare.at[step], partner
                        ).start()
                    copy(
                        kids.at[step, 0, lines],
                        kids.at[step, 1, lines],
                        send_kids.at[block],
                        recv_kids.at[step, block],
                        partner,
                    ).start()

                def hand_out_rows(first, count):
                    for t in range(first, first + count):
                        for g in range(2):
                            hand_out(t, 0, diag_passer(t, g))
                            hand_out(t, 1 + g, panel_passer(t, g))

                @pl.when(step == LEVELS - 1)
                def _():
                    hand_out_rows(4 * block, 4)

                if block == W // BLOCK - 1:

                    @pl.when(step < LEVELS - 1)
                    def _():
                        hand_out_rows(0, 16)

            with jax.named_scope("factor"):
                factor(mine, give)
            give(W // BLOCK - 1)

        return jnp.where(step == 0, 1, stride * 2), first // 2

    @pl.when(works)
    def _():
        lax.fori_loop(0, LEVELS, climb, (1, NODES - 1))

    @pl.when(passes_back)
    def _():
        with jax.named_scope("wait3"):
            for step in range(LEVELS):
                came_back(step)

        def unplace(s):
            back_label[s] = back_place[within(order[0, NODES + s])]

        for s in range(NODES):
            unplace(s)

    def hand_back(s, to, recv):
        copy(back_label.at[s], to, send4, recv, (s, 1 - grp)).start()

    for turn in range(4):

        @pl.when(on_diag & (tile % 4 == turn))
        def _(turn=turn):
            for s in NEAR_FIRST[turn]:
                hand_back(s, got_diag.at[rows(tile)], recv_diag)

        @pl.when(on_panel & (tile % 4 == turn))
        def _(turn=turn):
            for s in NEAR_FIRST[turn]:
                hand_back(s, got_panel.at[rows(tile)], recv_panel)

    sent = by_label.at[pl.ds(0, 24)]
    pltpu.make_async_copy(sent, sent, send1).wait()

    @pl.when(passes_in)
    def _():
        for step in range(4, LEVELS):
            later = by_place.at[pl.ds(0, 1 << (6 - step))]
            pltpu.make_async_copy(later, later, send2.at[step - 1]).wait()

    @pl.when(works)
    def _():
        def drain(step, stride):
            @pl.when(active(step, stride))
            def _():
                pltpu.make_async_copy(by_label, by_label, send3.at[step]).wait()

            return jnp.where(step == 0, 1, stride * 2)

        lax.fori_loop(0, LEVELS, drain, 1)

        @pl.when(role > 0)
        def _():
            for block in range(W // BLOCK):
                lines = kids.at[0, 0, pl.ds(BLOCK * block, BLOCK)]
                pltpu.make_async_copy(lines, lines, send_kids.at[block]).wait()
            pltpu.make_async_copy(spare.at[0], spare.at[0], send_spare).wait()

    @pl.when(passes_back)
    def _():
        pltpu.make_async_copy(back_label, back_label, send4).wait()

    with jax.named_scope("waitfinal"):
        pltpu.make_async_copy(got_diag, got_diag, recv_diag).wait()
        pltpu.make_async_copy(got_panel, got_panel, recv_panel).wait()
    down = lax.broadcasted_iota(jnp.int32, (W, W), 0)
    across = lax.broadcasted_iota(jnp.int32, (W, W), 1)
    out_diag[0] = jnp.where(across >= down, got_diag[...], 0.0).T
    out_panel[0, 0] = got_panel[...].T


def shards(diag_blocks, panel_blocks, targets):
    dma = pltpu.SemaphoreType.DMA
    tiles = pltpu.VMEM((NODES, 8, W), F32)
    return pl.pallas_call(
        tree_kernel,
        out_shape=(
            pltpu.VMEM(diag_blocks.shape, F32),
            pltpu.VMEM(panel_blocks.shape, F32),
        ),
        in_specs=[pl.BlockSpec(memory_space=pl.ANY)] * 3,
        out_specs=(pl.BlockSpec(memory_space=pltpu.VMEM),) * 2,
        scratch_shapes=[
            pltpu.VMEM((2, NODES), jnp.int32),
            pltpu.VMEM(diag_blocks.shape, F32),
            pltpu.VMEM(panel_blocks.shape, F32),
            pltpu.VMEM((W, W), F32),
            pltpu.VMEM((W, W), F32),
            pltpu.VMEM((W, W), F32),
            pltpu.VMEM((8, 2 * NODES), jnp.int32),
            pltpu.SMEM((8, 2 * NODES), jnp.int32),
            tiles,
            tiles,
            tiles,
            tiles,
            pltpu.VMEM((LEVELS, W, 3 * W), F32),
            pltpu.VMEM((LEVELS, 2, W, 2 * W), BF16),
            pltpu.VMEM((LEVELS, W, W), F32),
            pltpu.VMEM((LEVELS, W, W), F32),
            dma((4,)),
            dma,
            dma,
            dma((LEVELS - 1,)),
            dma((LEVELS,)),
            dma((W // BLOCK,)),
            dma((LEVELS, W // BLOCK)),
            dma,
            dma((LEVELS,)),
            dma((LEVELS,)),
            dma((LEVELS,)),
            dma,
            dma,
            dma,
        ],
        compiler_params=pltpu.CompilerParams(collective_id=0, has_side_effects=True),
        name="tree",
    )(targets.T, diag_blocks, panel_blocks)


def solution(mesh):
    placed = (P("col", None, None), P("col", "grp", None, None), P())
    return jax.shard_map(
        shards,
        mesh=mesh,
        in_specs=placed,
        out_specs=(P("col", None, None), P("col", "grp", None, None)),
        check_vma=False,
    )
```

```python
import jax
import jax.numpy as jnp
from jax import lax
from jax.experimental import pallas as pl
from jax.experimental.pallas import tpu as pltpu
from jax.sharding import PartitionSpec as P

F32, BF16 = jnp.float32, jnp.bfloat16
MESH = pl.DeviceIdType.MESH
W = 128
NODES = 64
LEVELS = 7
BLOCK = 32
NEAR_FIRST = tuple(
    tuple(sorted(range(NODES), key=lambda s: (s // 16 + s // 4 % 4 + s % 4, (s * 7 + 16 * turn) % NODES)))
    for turn in range(4)
)
PART = 16


def power_of_two(n, most):
    result = jnp.ones_like(n)
    for k in range(1, most + 1):
        result = result * jnp.where(n >= k, 2.0, 1.0)
    return result


def heap_order(parent):
    def dot(a, b, over):
        return lax.dot_general(
            a.astype(BF16), b.astype(BF16), ((over[:1], over[1:]), ((), ())), preferred_element_type=F32
        )

    down = lax.broadcasted_iota(jnp.int32, (NODES, NODES), 0)
    across = lax.broadcasted_iota(jnp.int32, (NODES, NODES), 1)
    one = (down == parent).astype(F32)
    two = dot(one, one, (1, 0))
    four = dot(two, two, (1, 0))
    alive = jnp.broadcast_to((parent < NODES).astype(F32), (8, NODES))
    len2 = alive + dot(alive, one, (1, 0))
    len4 = len2 + dot(len2, two, (1, 0))
    depth = len4 + dot(len4, four, (1, 0))
    path = (depth == LEVELS - 1).astype(F32)
    for above in (one, two, four):
        path = path + dot(path, above, (1, 1))
    siblings = dot(one, one, (0, 0))
    rank = jnp.sum(jnp.where(down < across, siblings, 0.0), axis=0, keepdims=True)
    beside = dot(path, siblings, (1, 0)) - path * alive
    code = alive * (1.0 - path) * jnp.maximum(beside, rank)
    code = code + (1.0 + alive) * dot(code, one, (1, 0))
    code = code + power_of_two(len2, 2) * dot(code, two, (1, 0))
    code = code + power_of_two(len4, 4) * dot(code, four, (1, 0))
    place = power_of_two(depth, LEVELS - 1) - 1.0 + code
    holds = (down == jnp.broadcast_to(place[:1], (NODES, NODES)).astype(jnp.int32)).astype(F32)
    label = lax.broadcasted_iota(jnp.int32, (8, NODES), 1).astype(F32)
    return dot(label, holds, (1, 1)), place


def in_three(x):
    high = x.astype(BF16)
    rest = x - high.astype(F32)
    middle = rest.astype(BF16)
    return high, middle, (rest - middle.astype(F32)).astype(BF16)


def wide(x, n):
    return jnp.concatenate([x] * n, axis=1)


def factor(work, after_block):
    tall = BLOCK // 8
    row = lax.broadcasted_iota(jnp.int32, (8, W), 0)

    def line(x, s):
        return jnp.broadcast_to(x[s : s + 1, :], (8, W))

    for b in range(W // BLOCK):
        start = b * BLOCK
        if b > 0:
            after_block(b - 1)
        x = [work[pl.ds(start + 8 * v, 8), :] for v in range(tall)]
        pivots = [None] * tall
        for part in range(0, BLOCK, PART):
            cols = {}
            for k in range(part, part + PART):
                lane = jnp.full((8, W), start + k, jnp.int32)
                for v in range(k // 8, tall):
                    cols[k, v] = jnp.take_along_axis(x[v][:, :W], lane, axis=1)
            d = line(cols[part, part // 8], part % 8)
            for j in range(part, part + PART):
                v0, s = divmod(j, 8)
                r = lax.rsqrt(d)
                r2 = r * r
                pivots[v0] = d if s == 0 else jnp.where(row == s, d, pivots[v0])
                mult = {v: cols[j, v] * r2 for v in range(v0, tall)}
                below = dict(mult)
                below[v0] = jnp.where(row > s, mult[v0], 0.0)
                across = {k: line(cols[j, k // 8], k % 8) for k in range(j + 1, part + PART)}
                if j + 1 < part + PART:
                    near = across[j + 1]
                    d = line(cols[j + 1, (j + 1) // 8], (j + 1) % 8) - (near * near) * r2
                for k in range(j + 1, part + PART):
                    for v in range(k // 8, tall):
                        cols[k, v] = cols[k, v] - mult[v] * across[k]
                pivot = jnp.concatenate([line(x[v0][:, c * W : (c + 1) * W], s) for c in range(3)], axis=1)
                for v in range(v0, tall):
                    x[v] = x[v] - wide(below[v], 3) * pivot
        for v in range(tall):
            x[v] = x[v] * wide(lax.rsqrt(pivots[v]), 3)
            work[pl.ds(start + 8 * v, 8), :] = x[v]
        if start + BLOCK < W:
            high, middle, low3 = in_three(jnp.concatenate(x, axis=0))
            right = jnp.concatenate([high, middle, high, low3, middle, high], axis=0)
            left = jnp.concatenate(
                [p[:, :W] for p in (high, high, middle, high, middle, low3)], axis=0
            )
            update = jnp.dot(left.T[start + BLOCK :, :], right, preferred_element_type=F32)
            work[pl.ds(start + BLOCK, W - start - BLOCK), :] -= update


def tree_kernel(
    targets_in,
    diag_in,
    panel_in,
    out_diag,
    out_panel,
    targets,
    diag,
    panel,
    turned,
    got_diag,
    got_panel,
    ranks,
    order,
    by_label,
    by_place,
    back_place,
    back_label,
    work,
    kids,
    spare,
    spare_in,
    load,
    send1,
    recv1,
    send2,
    recv2,
    send_kids,
    recv_kids,
    send_spare,
    recv_spare,
    send3,
    recv3,
    send4,
    recv_diag,
    recv_panel,
):
    col = lax.axis_index("col")
    grp = lax.axis_index("grp")
    y, x, z = col // 16, (col // 4) % 4, col % 4
    upper_z, upper_x = z // 2, x // 2
    works = (upper_z + upper_x) == 2
    role = (
        (1 - grp) + 2 * (z % 2) + 4 * (x % 2) + 8 * jnp.where(y % 3 == 0, 1, 0) + 16 * (y // 2)
    )
    tile = (z % 2) + 2 * (x % 2) + 4 * ((y + 2) % 4)
    on_diag = (upper_z + upper_x) == 0
    on_panel = ((upper_z + upper_x) == 1) & (upper_x == grp)
    passes_in = on_panel | (on_diag & ((tile < 8) == (grp == 1)))
    passes_back = on_panel | on_diag
    kind = jnp.where(on_panel, 2 - grp, 0)
    lanes = pl.ds(pl.multiple_of(W * kind, W), W)

    def at(dz, dx, t):
        return ((t // 4 + 2) % 4) * 16 + (2 * dx + (t // 2) % 2) * 4 + 2 * dz + t % 2

    def diag_passer(t, g):
        return (at(0, 0, t), g)

    def panel_passer(t, c):
        return (at(c, 1 - c, t), 1 - c)

    def worker(r):
        b3, b4 = (r // 8) % 2, r // 16
        wy = (1 - b4) * (1 - b3) + b4 * (2 + b3)
        return (wy * 16 + (2 + (r // 4) % 2) * 4 + 2 + (r // 2) % 2, 1 - r % 2)

    def within(n):
        return jnp.minimum(jnp.maximum(n, 0), NODES - 1)

    def rows(n):
        return pl.ds(pl.multiple_of(n * 8, 8), 8)

    def copy(src, dst, send, recv, to):
        return pltpu.make_async_remote_copy(
            src_ref=src, dst_ref=dst, send_sem=send, recv_sem=recv, device_id=to, device_id_type=MESH
        )

    def repeat(n, body, group=4):
        def several(i, carry):
            for k in range(group):
                body(i * group + k)
            return carry

        lax.fori_loop(0, n // group, several, 0)

    loads = [
        pltpu.make_async_copy(src, dst, load.at[k])
        for k, (src, dst) in enumerate(((targets_in, targets), (diag_in, diag), (panel_in, panel)))
    ]
    for one in loads:
        one.start()

    barrier = pltpu.get_barrier_semaphore()

    def greet(to):
        pl.semaphore_signal(barrier, inc=1, device_id=to, device_id_type=MESH)

    @pl.when(passes_in)
    def _():
        for s in NEAR_FIRST[0]:
            greet((s, 1 - grp))

    greet((col, 1 - grp))

    @pl.when(works)
    def _():
        kids[0] = jnp.zeros((2, W, 2 * W), BF16)
        spare[0] = jnp.zeros((W, W), F32)
        spare_in[0] = jnp.zeros((W, W), F32)

    loads[1].wait()
    loads[2].wait()
    turned[...] = panel[0, 0].T
    with jax.named_scope("barrier"):
        pl.semaphore_wait(barrier, 24 + 1)

    def spread_panel(i):
        t = (i + col) % 16
        copy(turned.at[rows(t)], by_label.at[col], send1, recv1, (at(grp, 1 - grp, t), 1 - grp)).start()

    def spread_diag(i):
        t = 8 * grp + (i + col) % 8
        copy(diag.at[0, rows(t)], by_label.at[col], send1, recv1, diag_passer(t, 1 - grp)).start()

    with jax.named_scope("spread"):
        repeat(8, spread_diag)
        repeat(16, spread_panel)

    loads[0].wait()

    @pl.when(passes_back)
    def _():
        with jax.named_scope("order"):
            node, place = heap_order(targets[0:1, :])
            ranks[:, :NODES] = node.astype(jnp.int32)
            ranks[:, NODES:] = place.astype(jnp.int32)
            to_scalar = pltpu.make_async_copy(ranks, order, load.at[3])
            to_scalar.start()
            to_scalar.wait()

    def came_back(step):
        tiles = back_place.at[pl.ds(0, 1 if step == 0 else 1 << (6 - step))]
        pltpu.make_async_copy(tiles, tiles, recv3.at[step]).wait()

    @pl.when(passes_in)
    def _():
        with jax.named_scope("wait1"):
            pltpu.make_async_copy(by_label, by_label, recv1).wait()

        def place(h):
            by_place[h] = by_label[within(order[0, h])]

        for h in range(NODES):
            place(h)

        def hand_in(step, h, r):
            copy(
                by_place.at[h], work.at[step, rows(tile), lanes], send2.at[max(step - 1, 0)], recv2.at[step], worker(r)
            ).start()

        with jax.named_scope("handin"):
            hand_in(0, NODES - 1, 0)
            for turn in range(4):

                @pl.when((tile + kind) % 4 == turn)
                def _(turn=turn):
                    for i in range(32):
                        r = (i + 8 * turn) % 32
                        hand_in(1, 31 + r, r)

            first = by_place.at[pl.ds(0, 33)]
            pltpu.make_async_copy(first, first, send2.at[0]).wait()
            for step in range(2, LEVELS):
                count = 1 << (6 - step)
                if step in (3, 4):
                    left = by_place.at[pl.ds(0, 2 * count)]
                    pltpu.make_async_copy(left, left, send2.at[step - 2]).wait()
                for r in range(count):
                    hand_in(step, count - 1 + r, r << (step - 1))

    def active(step, stride):
        return (role % stride == 0) & ((step > 0) | (role == 0))

    def climb(step, carry):
        stride, first = carry

        @pl.when(active(step, stride))
        def _():
            prev = jnp.maximum(step - 1, 0)
            gives = (role // stride) % 2 == 1
            partner = worker(jnp.maximum(role - stride, 0))
            place = first + role // stride
            mine = work.at[step]
            with jax.named_scope("waitheld"):
                pltpu.make_async_copy(mine, mine, recv2.at[step]).wait()

            @pl.when(step > 1)
            def _():
                with jax.named_scope("waitkids"):
                    pltpu.make_async_copy(spare_in.at[prev], spare_in.at[prev], recv_spare.at[prev]).wait()
                    for block in range(W // BLOCK):
                        lines = kids.at[prev, 1, pl.ds(BLOCK * block, BLOCK)]
                        pltpu.make_async_copy(lines, lines, recv_kids.at[prev, block]).wait()

            both = jnp.concatenate([kids[prev, 0], kids[prev, 1]], axis=0)
            update = jnp.dot(both[:, :W].T, both, preferred_element_type=F32)
            work[step, :, :W] -= update[:, :W] + (spare[prev] + spare_in[prev])
            work[step, :, W : 2 * W] -= update[:, W:]
            spare[step] = jnp.dot(both[:, W:].T, both[:, W:], preferred_element_type=F32)

            def hand_out(t, c, to):
                copy(
                    work.at[step, pl.ds(8 * t, 8), pl.ds(W * c, W)],
                    back_place.at[place],
                    send3.at[step],
                    recv3.at[step],
                    to,
                ).start()

            def give(block):
                lines = pl.ds(BLOCK * block, BLOCK)
                kids[step, 0, lines, :] = mine[lines, W:].astype(BF16)

                @pl.when(gives)
                def _():
                    if block == 0:
                        copy(
                            spare.at[step], spare_in.at[step], send_spare, recv_spare.at[step], partner
                        ).start()
                    copy(
                        kids.at[step, 0, lines],
                        kids.at[step, 1, lines],
                        send_kids.at[block],
                        recv_kids.at[step, block],
                        partner,
                    ).start()

                def hand_out_rows(first, count):
                    for t in range(first, first + count):
                        for g in range(2):
                            hand_out(t, 0, diag_passer(t, g))
                            hand_out(t, 1 + g, panel_passer(t, g))

                @pl.when(step == LEVELS - 1)
                def _():
                    hand_out_rows(4 * block, 4)

                if block == W // BLOCK - 1:

                    @pl.when(step < LEVELS - 1)
                    def _():
                        hand_out_rows(0, 16)

            with jax.named_scope("factor"):
                factor(mine, give)
            give(W // BLOCK - 1)

        return jnp.where(step == 0, 1, stride * 2), first // 2

    @pl.when(works)
    def _():
        lax.fori_loop(0, LEVELS, climb, (1, NODES - 1))

    @pl.when(passes_back)
    def _():
        with jax.named_scope("wait3"):
            for step in range(LEVELS):
                came_back(step)

        def unplace(s):
            back_label[s] = back_place[within(order[0, NODES + s])]

        for s in range(NODES):
            unplace(s)

    def hand_back(s, to, recv):
        copy(back_label.at[s], to, send4, recv, (s, 1 - grp)).start()

    for turn in range(4):

        @pl.when(on_diag & (tile % 4 == turn))
        def _(turn=turn):
            for s in NEAR_FIRST[turn]:
                hand_back(s, got_diag.at[rows(tile)], recv_diag)

        @pl.when(on_panel & (tile % 4 == turn))
        def _(turn=turn):
            for s in NEAR_FIRST[turn]:
                hand_back(s, got_panel.at[rows(tile)], recv_panel)

    sent = by_label.at[pl.ds(0, 24)]
    pltpu.make_async_copy(sent, sent, send1).wait()

    @pl.when(passes_in)
    def _():
        for step in range(4, LEVELS):
            later = by_place.at[pl.ds(0, 1 << (6 - step))]
            pltpu.make_async_copy(later, later, send2.at[step - 1]).wait()

    @pl.when(works)
    def _():
        def drain(step, stride):
            @pl.when(active(step, stride))
            def _():
                pltpu.make_async_copy(by_label, by_label, send3.at[step]).wait()

            return jnp.where(step == 0, 1, stride * 2)

        lax.fori_loop(0, LEVELS, drain, 1)

        @pl.when(role > 0)
        def _():
            for block in range(W // BLOCK):
                lines = kids.at[0, 0, pl.ds(BLOCK * block, BLOCK)]
                pltpu.make_async_copy(lines, lines, send_kids.at[block]).wait()
            pltpu.make_async_copy(spare.at[0], spare.at[0], send_spare).wait()

    @pl.when(passes_back)
    def _():
        pltpu.make_async_copy(back_label, back_label, send4).wait()

    with jax.named_scope("waitfinal"):
        pltpu.make_async_copy(got_diag, got_diag, recv_diag).wait()
        pltpu.make_async_copy(got_panel, got_panel, recv_panel).wait()
    down = lax.broadcasted_iota(jnp.int32, (W, W), 0)
    across = lax.broadcasted_iota(jnp.int32, (W, W), 1)
    out_diag[0] = jnp.where(across >= down, got_diag[...], 0.0).T
    out_panel[0, 0] = got_panel[...].T


def deliver_kernel(diag, panel, out_diag, out_panel, sems):
    copies = [
        pltpu.make_async_copy(diag, out_diag, sems.at[0]),
        pltpu.make_async_copy(panel, out_panel, sems.at[1]),
    ]
    for one in copies:
        one.start()
    for one in copies:
        one.wait()


def shards(diag_blocks, panel_blocks, targets):
    dma = pltpu.SemaphoreType.DMA
    tiles = pltpu.VMEM((NODES, 8, W), F32)
    factors = pl.pallas_call(
        tree_kernel,
        out_shape=(
            pltpu.VMEM(diag_blocks.shape, F32),
            pltpu.VMEM(panel_blocks.shape, F32),
        ),
        in_specs=[pl.BlockSpec(memory_space=pl.ANY)] * 3,
        out_specs=(pl.BlockSpec(memory_space=pltpu.VMEM),) * 2,
        scratch_shapes=[
            pltpu.VMEM((2, NODES), jnp.int32),
            pltpu.VMEM(diag_blocks.shape, F32),
            pltpu.VMEM(panel_blocks.shape, F32),
            pltpu.VMEM((W, W), F32),
            pltpu.VMEM((W, W), F32),
            pltpu.VMEM((W, W), F32),
            pltpu.VMEM((8, 2 * NODES), jnp.int32),
            pltpu.SMEM((8, 2 * NODES), jnp.int32),
            tiles,
            tiles,
            tiles,
            tiles,
            pltpu.VMEM((LEVELS, W, 3 * W), F32),
            pltpu.VMEM((LEVELS, 2, W, 2 * W), BF16),
            pltpu.VMEM((LEVELS, W, W), F32),
            pltpu.VMEM((LEVELS, W, W), F32),
            dma((4,)),
            dma,
            dma,
            dma((LEVELS - 1,)),
            dma((LEVELS,)),
            dma((W // BLOCK,)),
            dma((LEVELS, W // BLOCK)),
            dma,
            dma((LEVELS,)),
            dma((LEVELS,)),
            dma((LEVELS,)),
            dma,
            dma,
            dma,
        ],
        compiler_params=pltpu.CompilerParams(collective_id=0, has_side_effects=True),
        name="tree",
    )(targets.T, diag_blocks, panel_blocks)
    return pl.pallas_call(
        deliver_kernel,
        out_shape=tuple(jax.ShapeDtypeStruct(f.shape, F32) for f in factors),
        in_specs=(pl.BlockSpec(memory_space=pltpu.VMEM),) * 2,
        out_specs=(pl.BlockSpec(memory_space=pl.ANY),) * 2,
        scratch_shapes=[dma((2,))],
        name="deliver",
    )(*(pltpu.with_memory_space_constraint(f, pltpu.VMEM) for f in factors))


def solution(mesh):
    placed = (P("col", None, None), P("col", "grp", None, None), P())
    return jax.shard_map(
        shards,
        mesh=mesh,
        in_specs=placed,
        out_specs=(P("col", None, None), P("col", "grp", None, None)),
        check_vma=False,
    )
```

```python
import jax
import jax.numpy as jnp
from jax import lax
from jax.experimental import pallas as pl
from jax.experimental.pallas import tpu as pltpu
from jax.sharding import PartitionSpec as P

F32, BF16 = jnp.float32, jnp.bfloat16
MESH = pl.DeviceIdType.MESH
W = 128
NODES = 64
LEVELS = 7
BLOCK = 32
NEAR_FIRST = tuple(
    tuple(sorted(range(NODES), key=lambda s: (s // 16 + s // 4 % 4 + s % 4, (s * 7 + 16 * turn) % NODES)))
    for turn in range(4)
)
PART = 16


def power_of_two(n, most):
    result = jnp.ones_like(n)
    for k in range(1, most + 1):
        result = result * jnp.where(n >= k, 2.0, 1.0)
    return result


def heap_order(parent):
    def dot(a, b, over):
        return lax.dot_general(
            a.astype(BF16), b.astype(BF16), ((over[:1], over[1:]), ((), ())), preferred_element_type=F32
        )

    down = lax.broadcasted_iota(jnp.int32, (NODES, NODES), 0)
    across = lax.broadcasted_iota(jnp.int32, (NODES, NODES), 1)
    one = (down == parent).astype(F32)
    two = dot(one, one, (1, 0))
    four = dot(two, two, (1, 0))
    alive = jnp.broadcast_to((parent < NODES).astype(F32), (8, NODES))
    len2 = alive + dot(alive, one, (1, 0))
    len4 = len2 + dot(len2, two, (1, 0))
    depth = len4 + dot(len4, four, (1, 0))
    path = (depth == LEVELS - 1).astype(F32)
    for above in (one, two, four):
        path = path + dot(path, above, (1, 1))
    siblings = dot(one, one, (0, 0))
    rank = jnp.sum(jnp.where(down < across, siblings, 0.0), axis=0, keepdims=True)
    beside = dot(path, siblings, (1, 0)) - path * alive
    code = alive * (1.0 - path) * jnp.maximum(beside, rank)
    code = code + (1.0 + alive) * dot(code, one, (1, 0))
    code = code + power_of_two(len2, 2) * dot(code, two, (1, 0))
    code = code + power_of_two(len4, 4) * dot(code, four, (1, 0))
    place = power_of_two(depth, LEVELS - 1) - 1.0 + code
    holds = (down == jnp.broadcast_to(place[:1], (NODES, NODES)).astype(jnp.int32)).astype(F32)
    label = lax.broadcasted_iota(jnp.int32, (8, NODES), 1).astype(F32)
    return dot(label, holds, (1, 1)), place


def in_three(x):
    high = x.astype(BF16)
    rest = x - high.astype(F32)
    middle = rest.astype(BF16)
    return high, middle, (rest - middle.astype(F32)).astype(BF16)


def wide(x, n):
    return jnp.concatenate([x] * n, axis=1)


def factor(work, after_block):
    tall = BLOCK // 8
    row = lax.broadcasted_iota(jnp.int32, (8, W), 0)

    def line(x, s):
        return jnp.broadcast_to(x[s : s + 1, :], (8, W))

    for b in range(W // BLOCK):
        start = b * BLOCK
        if b > 0:
            after_block(b - 1)
        x = [work[pl.ds(start + 8 * v, 8), :] for v in range(tall)]
        pivots = [None] * tall
        for part in range(0, BLOCK, PART):
            cols = {}
            for k in range(part, part + PART):
                lane = jnp.full((8, W), start + k, jnp.int32)
                for v in range(k // 8, tall):
                    cols[k, v] = jnp.take_along_axis(x[v][:, :W], lane, axis=1)
            d = line(cols[part, part // 8], part % 8)
            for j in range(part, part + PART):
                v0, s = divmod(j, 8)
                r = lax.rsqrt(d)
                r2 = r * r
                pivots[v0] = d if s == 0 else jnp.where(row == s, d, pivots[v0])
                mult = {v: cols[j, v] * r2 for v in range(v0, tall)}
                below = dict(mult)
                below[v0] = jnp.where(row > s, mult[v0], 0.0)
                across = {k: line(cols[j, k // 8], k % 8) for k in range(j + 1, part + PART)}
                if j + 1 < part + PART:
                    near = across[j + 1]
                    d = line(cols[j + 1, (j + 1) // 8], (j + 1) % 8) - (near * near) * r2
                for k in range(j + 1, part + PART):
                    for v in range(k // 8, tall):
                        cols[k, v] = cols[k, v] - mult[v] * across[k]
                pivot = jnp.concatenate([line(x[v0][:, c * W : (c + 1) * W], s) for c in range(3)], axis=1)
                for v in range(v0, tall):
                    x[v] = x[v] - wide(below[v], 3) * pivot
        for v in range(tall):
            x[v] = x[v] * wide(lax.rsqrt(pivots[v]), 3)
            work[pl.ds(start + 8 * v, 8), :] = x[v]
        if start + BLOCK < W:
            high, middle, low3 = in_three(jnp.concatenate(x, axis=0))
            right = jnp.concatenate([high, middle, high, low3, middle, high], axis=0)
            left = jnp.concatenate(
                [p[:, :W] for p in (high, high, middle, high, middle, low3)], axis=0
            )
            update = jnp.dot(left.T[start + BLOCK :, :], right, preferred_element_type=F32)
            work[pl.ds(start + BLOCK, W - start - BLOCK), :] -= update


def tree_kernel(
    targets_in,
    diag_in,
    panel_in,
    out_diag,
    out_panel,
    targets,
    diag,
    panel,
    turned,
    got_diag,
    got_panel,
    ranks,
    order,
    by_label,
    by_place,
    back_place,
    back_label,
    work,
    kids,
    spare,
    spare_in,
    load,
    send1,
    recv1,
    send2,
    recv2,
    send_kids,
    recv_kids,
    send_spare,
    recv_spare,
    send3,
    recv3,
    send4,
    recv_diag,
    recv_panel,
):
    col = lax.axis_index("col")
    grp = lax.axis_index("grp")
    y, x, z = col // 16, (col // 4) % 4, col % 4
    upper_z, upper_x = z // 2, x // 2
    works = (upper_z + upper_x) == 2
    role = (
        (1 - grp) + 2 * (z % 2) + 4 * (x % 2) + 8 * jnp.where(y % 3 == 0, 1, 0) + 16 * (y // 2)
    )
    tile = (z % 2) + 2 * (x % 2) + 4 * ((y + 2) % 4)
    on_diag = (upper_z + upper_x) == 0
    on_panel = ((upper_z + upper_x) == 1) & (upper_x == grp)
    passes_in = on_panel | (on_diag & ((tile < 8) == (grp == 1)))
    passes_back = on_panel | on_diag
    kind = jnp.where(on_panel, 2 - grp, 0)
    lanes = pl.ds(pl.multiple_of(W * kind, W), W)

    def at(dz, dx, t):
        return ((t // 4 + 2) % 4) * 16 + (2 * dx + (t // 2) % 2) * 4 + 2 * dz + t % 2

    def diag_passer(t, g):
        return (at(0, 0, t), g)

    def panel_passer(t, c):
        return (at(c, 1 - c, t), 1 - c)

    def worker(r):
        b3, b4 = (r // 8) % 2, r // 16
        wy = (1 - b4) * (1 - b3) + b4 * (2 + b3)
        return (wy * 16 + (2 + (r // 4) % 2) * 4 + 2 + (r // 2) % 2, 1 - r % 2)

    def within(n):
        return jnp.minimum(jnp.maximum(n, 0), NODES - 1)

    def rows(n):
        return pl.ds(pl.multiple_of(n * 8, 8), 8)

    def copy(src, dst, send, recv, to):
        return pltpu.make_async_remote_copy(
            src_ref=src, dst_ref=dst, send_sem=send, recv_sem=recv, device_id=to, device_id_type=MESH
        )

    def repeat(n, body, group=4):
        def several(i, carry):
            for k in range(group):
                body(i * group + k)
            return carry

        lax.fori_loop(0, n // group, several, 0)

    loads = [
        pltpu.make_async_copy(src, dst, load.at[k])
        for k, (src, dst) in enumerate(((targets_in, targets), (diag_in, diag), (panel_in, panel)))
    ]
    for one in loads:
        one.start()

    barrier = pltpu.get_barrier_semaphore()

    def greet(to):
        pl.semaphore_signal(barrier, inc=1, device_id=to, device_id_type=MESH)

    @pl.when(passes_in)
    def _():
        for s in NEAR_FIRST[0]:
            greet((s, 1 - grp))

    greet((col, 1 - grp))

    @pl.when(works)
    def _():
        kids[0] = jnp.zeros((2, W, 2 * W), BF16)
        spare[0] = jnp.zeros((W, W), F32)
        spare_in[0] = jnp.zeros((W, W), F32)

    loads[1].wait()
    loads[2].wait()
    turned[...] = panel[0, 0].T
    with jax.named_scope("barrier"):
        pl.semaphore_wait(barrier, 24 + 1)

    def spread_panel(i):
        t = (i + col) % 16
        copy(turned.at[rows(t)], by_label.at[col], send1, recv1, (at(grp, 1 - grp, t), 1 - grp)).start()

    def spread_diag(i):
        t = 8 * grp + (i + col) % 8
        copy(diag.at[0, rows(t)], by_label.at[col], send1, recv1, diag_passer(t, 1 - grp)).start()

    with jax.named_scope("spread"):
        repeat(8, spread_diag)
        repeat(16, spread_panel)

    loads[0].wait()

    @pl.when(passes_back)
    def _():
        with jax.named_scope("order"):
            node, place = heap_order(targets[0:1, :])
            ranks[:, :NODES] = node.astype(jnp.int32)
            ranks[:, NODES:] = place.astype(jnp.int32)
            to_scalar = pltpu.make_async_copy(ranks, order, load.at[3])
            to_scalar.start()
            to_scalar.wait()

    @pl.when(passes_in)
    def _():
        with jax.named_scope("wait1"):
            pltpu.make_async_copy(by_label, by_label, recv1).wait()

        def place(h):
            by_place[h] = by_label[within(order[0, h])]

        for h in range(NODES):
            place(h)

        def hand_in(step, h, r):
            copy(
                by_place.at[h], work.at[step, rows(tile), lanes], send2.at[min(max(step - 1, 0), 3)], recv2.at[step], worker(r)
            ).start()

        with jax.named_scope("handin"):
            hand_in(0, NODES - 1, 0)
            for turn in range(4):

                @pl.when((tile + kind) % 4 == turn)
                def _(turn=turn):
                    for i in range(32):
                        r = (i + 8 * turn) % 32
                        hand_in(1, 31 + r, r)

            first = by_place.at[pl.ds(0, 33)]
            pltpu.make_async_copy(first, first, send2.at[0]).wait()
            for step in range(2, LEVELS):
                count = 1 << (6 - step)
                if step in (3, 4):
                    left = by_place.at[pl.ds(0, 2 * count)]
                    pltpu.make_async_copy(left, left, send2.at[step - 2]).wait()
                for r in range(count):
                    hand_in(step, count - 1 + r, r << (step - 1))

    def active(step, stride):
        return (role % stride == 0) & ((step > 0) | (role == 0))

    def climb(step, carry):
        stride, first = carry

        @pl.when(active(step, stride))
        def _():
            prev = jnp.maximum(step - 1, 0)
            gives = (role // stride) % 2 == 1
            partner = worker(jnp.maximum(role - stride, 0))
            given = jnp.maximum(step - 1, 0)
            place = first + role // stride
            mine = work.at[step]
            with jax.named_scope("waitheld"):
                pltpu.make_async_copy(mine, mine, recv2.at[step]).wait()

            @pl.when(step > 1)
            def _():
                with jax.named_scope("waitkids"):
                    pltpu.make_async_copy(spare_in.at[prev], spare_in.at[prev], recv_spare.at[prev - 1]).wait()
                    pltpu.make_async_copy(kids.at[prev, 1], kids.at[prev, 1], recv_kids.at[prev - 1]).wait()

            both = jnp.concatenate([kids[prev, 0], kids[prev, 1]], axis=0)
            update = jnp.dot(both[:, :W].T, both, preferred_element_type=F32)
            work[step, :, :W] -= update[:, :W] + (spare[prev] + spare_in[prev])
            work[step, :, W : 2 * W] -= update[:, W:]
            spare[step] = jnp.dot(both[:, W:].T, both[:, W:], preferred_element_type=F32)

            def hand_out(t, c, to):
                copy(
                    work.at[step, pl.ds(8 * t, 8), pl.ds(W * c, W)],
                    back_place.at[place],
                    send3.at[step],
                    recv3,
                    to,
                ).start()

            def give(block):
                lines = pl.ds(BLOCK * block, BLOCK)
                kids[step, 0, lines, :] = mine[lines, W:].astype(BF16)

                @pl.when(gives)
                def _():
                    if block == 0:
                        copy(
                            spare.at[step], spare_in.at[step], send_spare, recv_spare.at[given], partner
                        ).start()
                    copy(
                        kids.at[step, 0, lines],
                        kids.at[step, 1, lines],
                        send_kids,
                        recv_kids.at[given],
                        partner,
                    ).start()

                def hand_out_rows(first, count):
                    for t in range(first, first + count):
                        for g in range(2):
                            hand_out(t, 0, diag_passer(t, g))
                            hand_out(t, 1 + g, panel_passer(t, g))

                @pl.when(step == LEVELS - 1)
                def _():
                    hand_out_rows(4 * block, 4)

                if block == W // BLOCK - 1:

                    @pl.when(step < LEVELS - 1)
                    def _():
                        hand_out_rows(0, 16)

            with jax.named_scope("factor"):
                factor(mine, give)
            give(W // BLOCK - 1)

        return jnp.where(step == 0, 1, stride * 2), first // 2

    @pl.when(works)
    def _():
        lax.fori_loop(0, LEVELS, climb, (1, NODES - 1))

    @pl.when(passes_back)
    def _():
        with jax.named_scope("wait3"):
            pltpu.make_async_copy(back_place, back_place, recv3).wait()

        def unplace(s):
            back_label[s] = back_place[within(order[0, NODES + s])]

        for s in range(NODES):
            unplace(s)

    def hand_back(s, to, recv):
        copy(back_label.at[s], to, send4, recv, (s, 1 - grp)).start()

    for turn in range(4):

        @pl.when(on_diag & (tile % 4 == turn))
        def _(turn=turn):
            for s in NEAR_FIRST[turn]:
                hand_back(s, got_diag.at[rows(tile)], recv_diag)

        @pl.when(on_panel & (tile % 4 == turn))
        def _(turn=turn):
            for s in NEAR_FIRST[turn]:
                hand_back(s, got_panel.at[rows(tile)], recv_panel)

    sent = by_label.at[pl.ds(0, 24)]
    pltpu.make_async_copy(sent, sent, send1).wait()

    @pl.when(passes_in)
    def _():
        later = by_place.at[pl.ds(0, 7)]
        pltpu.make_async_copy(later, later, send2.at[3]).wait()

    @pl.when(works)
    def _():
        def drain(step, stride):
            @pl.when(active(step, stride))
            def _():
                pltpu.make_async_copy(by_label, by_label, send3.at[step]).wait()

            return jnp.where(step == 0, 1, stride * 2)

        lax.fori_loop(0, LEVELS, drain, 1)

        @pl.when(role > 0)
        def _():
            pltpu.make_async_copy(kids.at[0, 0], kids.at[0, 0], send_kids).wait()
            pltpu.make_async_copy(spare.at[0], spare.at[0], send_spare).wait()

    @pl.when(passes_back)
    def _():
        pltpu.make_async_copy(back_label, back_label, send4).wait()

    with jax.named_scope("waitfinal"):
        pltpu.make_async_copy(got_diag, got_diag, recv_diag).wait()
        pltpu.make_async_copy(got_panel, got_panel, recv_panel).wait()
    down = lax.broadcasted_iota(jnp.int32, (W, W), 0)
    across = lax.broadcasted_iota(jnp.int32, (W, W), 1)
    out_diag[0] = jnp.where(across >= down, got_diag[...], 0.0).T
    out_panel[0, 0] = got_panel[...].T


def deliver_kernel(diag, panel, out_diag, out_panel, sems):
    copies = [
        pltpu.make_async_copy(diag, out_diag, sems.at[0]),
        pltpu.make_async_copy(panel, out_panel, sems.at[1]),
    ]
    for one in copies:
        one.start()
    for one in copies:
        one.wait()


def shards(diag_blocks, panel_blocks, targets):
    dma = pltpu.SemaphoreType.DMA
    tiles = pltpu.VMEM((NODES, 8, W), F32)
    factors = pl.pallas_call(
        tree_kernel,
        out_shape=(
            pltpu.VMEM(diag_blocks.shape, F32),
            pltpu.VMEM(panel_blocks.shape, F32),
        ),
        in_specs=[pl.BlockSpec(memory_space=pl.ANY)] * 3,
        out_specs=(pl.BlockSpec(memory_space=pltpu.VMEM),) * 2,
        scratch_shapes=[
            pltpu.VMEM((2, NODES), jnp.int32),
            pltpu.VMEM(diag_blocks.shape, F32),
            pltpu.VMEM(panel_blocks.shape, F32),
            pltpu.VMEM((W, W), F32),
            pltpu.VMEM((W, W), F32),
            pltpu.VMEM((W, W), F32),
            pltpu.VMEM((8, 2 * NODES), jnp.int32),
            pltpu.SMEM((8, 2 * NODES), jnp.int32),
            tiles,
            tiles,
            tiles,
            tiles,
            pltpu.VMEM((LEVELS, W, 3 * W), F32),
            pltpu.VMEM((LEVELS, 2, W, 2 * W), BF16),
            pltpu.VMEM((LEVELS, W, W), F32),
            pltpu.VMEM((LEVELS, W, W), F32),
            dma((4,)),
            dma,
            dma,
            dma((4,)),
            dma((LEVELS,)),
            dma,
            dma((LEVELS - 2,)),
            dma,
            dma((LEVELS - 2,)),
            dma((LEVELS,)),
            dma,
            dma,
            dma,
            dma,
        ],
        compiler_params=pltpu.CompilerParams(collective_id=0, has_side_effects=True),
        name="tree",
    )(targets.T, diag_blocks, panel_blocks)
    return pl.pallas_call(
        deliver_kernel,
        out_shape=tuple(jax.ShapeDtypeStruct(f.shape, F32) for f in factors),
        in_specs=(pl.BlockSpec(memory_space=pltpu.VMEM),) * 2,
        out_specs=(pl.BlockSpec(memory_space=pl.ANY),) * 2,
        scratch_shapes=[dma((2,))],
        name="deliver",
    )(*(pltpu.with_memory_space_constraint(f, pltpu.VMEM) for f in factors))


def solution(mesh):
    placed = (P("col", None, None), P("col", "grp", None, None), P())
    return jax.shard_map(
        shards,
        mesh=mesh,
        in_specs=placed,
        out_specs=(P("col", None, None), P("col", "grp", None, None)),
        check_vma=False,
    )
```

```python
import jax
import jax.numpy as jnp
from jax import lax
from jax.experimental import pallas as pl
from jax.experimental.pallas import tpu as pltpu
from jax.sharding import PartitionSpec as P

F32, BF16 = jnp.float32, jnp.bfloat16
MESH = pl.DeviceIdType.MESH
W = 128
NODES = 64
LEVELS = 7
BLOCK = 32
NEAR_FIRST = tuple(
    tuple(sorted(range(NODES), key=lambda s: (s // 16 + s // 4 % 4 + s % 4, (s * 7 + 16 * turn) % NODES)))
    for turn in range(4)
)
PART = 16


def power_of_two(n, most):
    result = jnp.ones_like(n)
    for k in range(1, most + 1):
        result = result * jnp.where(n >= k, 2.0, 1.0)
    return result


def heap_order(parent):
    def dot(a, b, over):
        return lax.dot_general(
            a.astype(BF16), b.astype(BF16), ((over[:1], over[1:]), ((), ())), preferred_element_type=F32
        )

    down = lax.broadcasted_iota(jnp.int32, (NODES, NODES), 0)
    across = lax.broadcasted_iota(jnp.int32, (NODES, NODES), 1)
    one = (down == parent).astype(F32)
    two = dot(one, one, (1, 0))
    four = dot(two, two, (1, 0))
    alive = jnp.broadcast_to((parent < NODES).astype(F32), (8, NODES))
    len2 = alive + dot(alive, one, (1, 0))
    len4 = len2 + dot(len2, two, (1, 0))
    depth = len4 + dot(len4, four, (1, 0))
    path = (depth == LEVELS - 1).astype(F32)
    for above in (one, two, four):
        path = path + dot(path, above, (1, 1))
    siblings = dot(one, one, (0, 0))
    rank = jnp.sum(jnp.where(down < across, siblings, 0.0), axis=0, keepdims=True)
    beside = dot(path, siblings, (1, 0)) - path * alive
    code = alive * (1.0 - path) * jnp.maximum(beside, rank)
    code = code + (1.0 + alive) * dot(code, one, (1, 0))
    code = code + power_of_two(len2, 2) * dot(code, two, (1, 0))
    code = code + power_of_two(len4, 4) * dot(code, four, (1, 0))
    place = power_of_two(depth, LEVELS - 1) - 1.0 + code
    holds = (down == jnp.broadcast_to(place[:1], (NODES, NODES)).astype(jnp.int32)).astype(F32)
    label = lax.broadcasted_iota(jnp.int32, (8, NODES), 1).astype(F32)
    return dot(label, holds, (1, 1)), place


def in_three(x):
    high = x.astype(BF16)
    rest = x - high.astype(F32)
    middle = rest.astype(BF16)
    return high, middle, (rest - middle.astype(F32)).astype(BF16)


def wide(x, n):
    return jnp.concatenate([x] * n, axis=1)


def factor(work, after_block):
    tall = BLOCK // 8
    row = lax.broadcasted_iota(jnp.int32, (8, W), 0)

    def line(x, s):
        return jnp.broadcast_to(x[s : s + 1, :], (8, W))

    for b in range(W // BLOCK):
        start = b * BLOCK
        if b > 0:
            after_block(b - 1)
        x = [work[pl.ds(start + 8 * v, 8), :] for v in range(tall)]
        pivots = [None] * tall
        for part in range(0, BLOCK, PART):
            cols = {}
            for k in range(part, part + PART):
                lane = jnp.full((8, W), start + k, jnp.int32)
                for v in range(k // 8, tall):
                    cols[k, v] = jnp.take_along_axis(x[v][:, :W], lane, axis=1)
            d = line(cols[part, part // 8], part % 8)
            for j in range(part, part + PART):
                v0, s = divmod(j, 8)
                r = lax.rsqrt(d)
                r2 = r * r
                pivots[v0] = d if s == 0 else jnp.where(row == s, d, pivots[v0])
                mult = {v: cols[j, v] * r2 for v in range(v0, tall)}
                below = dict(mult)
                below[v0] = jnp.where(row > s, mult[v0], 0.0)
                across = {k: line(cols[j, k // 8], k % 8) for k in range(j + 1, part + PART)}
                if j + 1 < part + PART:
                    near = across[j + 1]
                    d = line(cols[j + 1, (j + 1) // 8], (j + 1) % 8) - (near * near) * r2
                for k in range(j + 1, part + PART):
                    for v in range(k // 8, tall):
                        cols[k, v] = cols[k, v] - mult[v] * across[k]
                pivot = jnp.concatenate([line(x[v0][:, c * W : (c + 1) * W], s) for c in range(3)], axis=1)
                for v in range(v0, tall):
                    x[v] = x[v] - wide(below[v], 3) * pivot
        for v in range(tall):
            x[v] = x[v] * wide(lax.rsqrt(pivots[v]), 3)
            work[pl.ds(start + 8 * v, 8), :] = x[v]
        if start + BLOCK < W:
            high, middle, low3 = in_three(jnp.concatenate(x, axis=0))
            right = jnp.concatenate([high, middle, high, low3, middle, high], axis=0)
            left = jnp.concatenate(
                [p[:, :W] for p in (high, high, middle, high, middle, low3)], axis=0
            )
            update = jnp.dot(left.T[start + BLOCK :, :], right, preferred_element_type=F32)
            work[pl.ds(start + BLOCK, W - start - BLOCK), :] -= update


def tree_kernel(
    targets_in,
    diag_in,
    panel_in,
    got_diag,
    got_panel,
    targets,
    diag,
    panel,
    turned,
    ranks,
    order,
    by_label,
    by_place,
    back_place,
    back_label,
    work,
    kids,
    spare,
    spare_in,
    load,
    send1,
    recv1,
    send2,
    recv2,
    send_kids,
    recv_kids,
    send_spare,
    recv_spare,
    send3,
    recv3,
    send4,
    recv_diag,
    recv_panel,
):
    col = lax.axis_index("col")
    grp = lax.axis_index("grp")
    y, x, z = col // 16, (col // 4) % 4, col % 4
    upper_z, upper_x = z // 2, x // 2
    works = (upper_z + upper_x) == 2
    role = (
        (1 - grp) + 2 * (z % 2) + 4 * (x % 2) + 8 * jnp.where(y % 3 == 0, 1, 0) + 16 * (y // 2)
    )
    tile = (z % 2) + 2 * (x % 2) + 4 * ((y + 2) % 4)
    on_diag = (upper_z + upper_x) == 0
    on_panel = ((upper_z + upper_x) == 1) & (upper_x == grp)
    passes_in = on_panel | (on_diag & ((tile < 8) == (grp == 1)))
    passes_back = on_panel | on_diag
    kind = jnp.where(on_panel, 2 - grp, 0)
    lanes = pl.ds(pl.multiple_of(W * kind, W), W)

    def at(dz, dx, t):
        return ((t // 4 + 2) % 4) * 16 + (2 * dx + (t // 2) % 2) * 4 + 2 * dz + t % 2

    def diag_passer(t, g):
        return (at(0, 0, t), g)

    def panel_passer(t, c):
        return (at(c, 1 - c, t), 1 - c)

    def worker(r):
        b3, b4 = (r // 8) % 2, r // 16
        wy = (1 - b4) * (1 - b3) + b4 * (2 + b3)
        return (wy * 16 + (2 + (r // 4) % 2) * 4 + 2 + (r // 2) % 2, 1 - r % 2)

    def within(n):
        return jnp.minimum(jnp.maximum(n, 0), NODES - 1)

    def rows(n):
        return pl.ds(pl.multiple_of(n * 8, 8), 8)

    def copy(src, dst, send, recv, to):
        return pltpu.make_async_remote_copy(
            src_ref=src, dst_ref=dst, send_sem=send, recv_sem=recv, device_id=to, device_id_type=MESH
        )

    def repeat(n, body, group=4):
        def several(i, carry):
            for k in range(group):
                body(i * group + k)
            return carry

        lax.fori_loop(0, n // group, several, 0)

    loads = [
        pltpu.make_async_copy(src, dst, load.at[k])
        for k, (src, dst) in enumerate(((targets_in, targets), (diag_in, diag), (panel_in, panel)))
    ]
    for one in loads:
        one.start()

    barrier = pltpu.get_barrier_semaphore()

    def greet(to):
        pl.semaphore_signal(barrier, inc=1, device_id=to, device_id_type=MESH)

    @pl.when(passes_in)
    def _():
        for s in NEAR_FIRST[0]:
            greet((s, 1 - grp))

    greet((col, 1 - grp))

    @pl.when(works)
    def _():
        kids[0] = jnp.zeros((2, W, 2 * W), BF16)
        spare[0] = jnp.zeros((W, W), F32)
        spare_in[0] = jnp.zeros((W, W), F32)

    loads[1].wait()
    loads[2].wait()
    turned[...] = panel[0, 0].T
    with jax.named_scope("barrier"):
        pl.semaphore_wait(barrier, 24 + 1)

    def spread_panel(i):
        t = (i + col) % 16
        copy(turned.at[rows(t)], by_label.at[col], send1, recv1, (at(grp, 1 - grp, t), 1 - grp)).start()

    def spread_diag(i):
        t = 8 * grp + (i + col) % 8
        copy(diag.at[0, rows(t)], by_label.at[col], send1, recv1, diag_passer(t, 1 - grp)).start()

    with jax.named_scope("spread"):
        repeat(8, spread_diag)
        repeat(16, spread_panel)

    loads[0].wait()

    @pl.when(passes_back)
    def _():
        with jax.named_scope("order"):
            node, place = heap_order(targets[0:1, :])
            ranks[:, :NODES] = node.astype(jnp.int32)
            ranks[:, NODES:] = place.astype(jnp.int32)
            to_scalar = pltpu.make_async_copy(ranks, order, load.at[3])
            to_scalar.start()
            to_scalar.wait()

    @pl.when(passes_in)
    def _():
        with jax.named_scope("wait1"):
            pltpu.make_async_copy(by_label, by_label, recv1).wait()

        def place(h):
            by_place[h] = by_label[within(order[0, h])]

        for h in range(NODES):
            place(h)

        def hand_in(step, h, r):
            copy(
                by_place.at[h], work.at[step, rows(tile), lanes], send2.at[min(max(step - 1, 0), 3)], recv2.at[step], worker(r)
            ).start()

        with jax.named_scope("handin"):
            hand_in(0, NODES - 1, 0)
            for turn in range(4):

                @pl.when((tile + kind) % 4 == turn)
                def _(turn=turn):
                    for i in range(32):
                        r = (i + 8 * turn) % 32
                        hand_in(1, 31 + r, r)

            first = by_place.at[pl.ds(0, 33)]
            pltpu.make_async_copy(first, first, send2.at[0]).wait()
            for step in range(2, LEVELS):
                count = 1 << (6 - step)
                if step in (3, 4):
                    left = by_place.at[pl.ds(0, 2 * count)]
                    pltpu.make_async_copy(left, left, send2.at[step - 2]).wait()
                for r in range(count):
                    hand_in(step, count - 1 + r, r << (step - 1))

    def active(step, stride):
        return (role % stride == 0) & ((step > 0) | (role == 0))

    def climb(step, carry):
        stride, first = carry

        @pl.when(active(step, stride))
        def _():
            prev = jnp.maximum(step - 1, 0)
            gives = (role // stride) % 2 == 1
            partner = worker(jnp.maximum(role - stride, 0))
            given = jnp.maximum(step - 1, 0)
            place = first + role // stride
            mine = work.at[step]
            with jax.named_scope("waitheld"):
                pltpu.make_async_copy(mine, mine, recv2.at[step]).wait()

            @pl.when(step > 1)
            def _():
                with jax.named_scope("waitkids"):
                    pltpu.make_async_copy(spare_in.at[prev], spare_in.at[prev], recv_spare.at[prev - 1]).wait()
                    pltpu.make_async_copy(kids.at[prev, 1], kids.at[prev, 1], recv_kids.at[prev - 1]).wait()

            both = jnp.concatenate([kids[prev, 0], kids[prev, 1]], axis=0)
            update = jnp.dot(both[:, :W].T, both, preferred_element_type=F32)
            work[step, :, :W] -= update[:, :W] + (spare[prev] + spare_in[prev])
            work[step, :, W : 2 * W] -= update[:, W:]
            spare[step] = jnp.dot(both[:, W:].T, both[:, W:], preferred_element_type=F32)

            def hand_out(t, c, to):
                copy(
                    work.at[step, pl.ds(8 * t, 8), pl.ds(W * c, W)],
                    back_place.at[place],
                    send3.at[step],
                    recv3,
                    to,
                ).start()

            def give(block):
                lines = pl.ds(BLOCK * block, BLOCK)
                kids[step, 0, lines, :] = mine[lines, W:].astype(BF16)

                @pl.when(gives)
                def _():
                    if block == 0:
                        copy(
                            spare.at[step], spare_in.at[step], send_spare, recv_spare.at[given], partner
                        ).start()
                    copy(
                        kids.at[step, 0, lines],
                        kids.at[step, 1, lines],
                        send_kids,
                        recv_kids.at[given],
                        partner,
                    ).start()

                def hand_out_rows(first, count):
                    for t in range(first, first + count):
                        for g in range(2):
                            hand_out(t, 0, diag_passer(t, g))
                            hand_out(t, 1 + g, panel_passer(t, g))

                @pl.when(step == LEVELS - 1)
                def _():
                    hand_out_rows(4 * block, 4)

                if block == W // BLOCK - 1:

                    @pl.when(step < LEVELS - 1)
                    def _():
                        hand_out_rows(0, 16)

            with jax.named_scope("factor"):
                factor(mine, give)
            give(W // BLOCK - 1)

        return jnp.where(step == 0, 1, stride * 2), first // 2

    @pl.when(works)
    def _():
        lax.fori_loop(0, LEVELS, climb, (1, NODES - 1))

    @pl.when(passes_back)
    def _():
        with jax.named_scope("wait3"):
            pltpu.make_async_copy(back_place, back_place, recv3).wait()

        def unplace(s):
            back_label[s] = back_place[within(order[0, NODES + s])]

        for s in range(NODES):
            unplace(s)

    def hand_back(s, to, recv):
        copy(back_label.at[s], to, send4, recv, (s, 1 - grp)).start()

    for turn in range(4):

        @pl.when(on_diag & (tile % 4 == turn))
        def _(turn=turn):
            for s in NEAR_FIRST[turn]:
                hand_back(s, got_diag.at[0, rows(tile)], recv_diag)

        @pl.when(on_panel & (tile % 4 == turn))
        def _(turn=turn):
            for s in NEAR_FIRST[turn]:
                hand_back(s, got_panel.at[0, 0, rows(tile)], recv_panel)

    sent = by_label.at[pl.ds(0, 24)]
    pltpu.make_async_copy(sent, sent, send1).wait()

    @pl.when(passes_in)
    def _():
        later = by_place.at[pl.ds(0, 7)]
        pltpu.make_async_copy(later, later, send2.at[3]).wait()

    @pl.when(works)
    def _():
        def drain(step, stride):
            @pl.when(active(step, stride))
            def _():
                pltpu.make_async_copy(by_label, by_label, send3.at[step]).wait()

            return jnp.where(step == 0, 1, stride * 2)

        lax.fori_loop(0, LEVELS, drain, 1)

        @pl.when(role > 0)
        def _():
            pltpu.make_async_copy(kids.at[0, 0], kids.at[0, 0], send_kids).wait()
            pltpu.make_async_copy(spare.at[0], spare.at[0], send_spare).wait()

    @pl.when(passes_back)
    def _():
        pltpu.make_async_copy(back_label, back_label, send4).wait()

    with jax.named_scope("waitfinal"):
        pltpu.make_async_copy(got_diag, got_diag, recv_diag).wait()
        pltpu.make_async_copy(got_panel, got_panel, recv_panel).wait()


def deliver_kernel(diag, panel, out_diag, out_panel, turned, sems):
    down = lax.broadcasted_iota(jnp.int32, (W, W), 0)
    across = lax.broadcasted_iota(jnp.int32, (W, W), 1)
    copies = [
        pltpu.make_async_copy(turned.at[0], out_diag.at[0], sems.at[0]),
        pltpu.make_async_copy(turned.at[1], out_panel.at[0, 0], sems.at[1]),
    ]
    turned[0] = jnp.where(across >= down, diag[0], 0.0).T
    copies[0].start()
    turned[1] = panel[0, 0].T
    copies[1].start()
    for one in copies:
        one.wait()


def shards(diag_blocks, panel_blocks, targets):
    dma = pltpu.SemaphoreType.DMA
    tiles = pltpu.VMEM((NODES, 8, W), F32)
    factors = pl.pallas_call(
        tree_kernel,
        out_shape=(
            pltpu.VMEM(diag_blocks.shape, F32),
            pltpu.VMEM(panel_blocks.shape, F32),
        ),
        in_specs=[pl.BlockSpec(memory_space=pl.ANY)] * 3,
        out_specs=(pl.BlockSpec(memory_space=pltpu.VMEM),) * 2,
        scratch_shapes=[
            pltpu.VMEM((2, NODES), jnp.int32),
            pltpu.VMEM(diag_blocks.shape, F32),
            pltpu.VMEM(panel_blocks.shape, F32),
            pltpu.VMEM((W, W), F32),
            pltpu.VMEM((8, 2 * NODES), jnp.int32),
            pltpu.SMEM((8, 2 * NODES), jnp.int32),
            tiles,
            tiles,
            tiles,
            tiles,
            pltpu.VMEM((LEVELS, W, 3 * W), F32),
            pltpu.VMEM((LEVELS, 2, W, 2 * W), BF16),
            pltpu.VMEM((LEVELS, W, W), F32),
            pltpu.VMEM((LEVELS, W, W), F32),
            dma((4,)),
            dma,
            dma,
            dma((4,)),
            dma((LEVELS,)),
            dma,
            dma((LEVELS - 2,)),
            dma,
            dma((LEVELS - 2,)),
            dma((LEVELS,)),
            dma,
            dma,
            dma,
            dma,
        ],
        compiler_params=pltpu.CompilerParams(collective_id=0, has_side_effects=True),
        name="tree",
    )(targets.T, diag_blocks, panel_blocks)
    return pl.pallas_call(
        deliver_kernel,
        out_shape=tuple(jax.ShapeDtypeStruct(f.shape, F32) for f in factors),
        in_specs=(pl.BlockSpec(memory_space=pltpu.VMEM),) * 2,
        out_specs=(pl.BlockSpec(memory_space=pl.ANY),) * 2,
        scratch_shapes=[pltpu.VMEM((2, W, W), F32), dma((2,))],
        name="deliver",
    )(*(pltpu.with_memory_space_constraint(f, pltpu.VMEM) for f in factors))


def solution(mesh):
    placed = (P("col", None, None), P("col", "grp", None, None), P())
    return jax.shard_map(
        shards,
        mesh=mesh,
        in_specs=placed,
        out_specs=(P("col", None, None), P("col", "grp", None, None)),
        check_vma=False,
    )
```
